32 devices in a mesh: ta: 4 (over y, core), gx: 2 (over x), gy: 4 (over z).
Axes of the slice: x: 2, y: 2, z: 4, core: 2. Of those that a mesh axis runs over, the one named last changes fastest.
Arguments:
- space_links: float32 [3, 2, 3, 3, 4, 4, 2304], P(None, None, None, None, 'ta', 'gx', 'gy'), may hold values from -1 to 1, as said below
- time_links: float32 [2, 3, 3, 4, 4, 2304], P(None, None, None, 'ta', 'gx', 'gy'), may hold values from -1 to 1, as said below
- start_gauge: float32 [2, 3, 3, 4, 4, 2304], P(None, None, None, 'ta', 'gx', 'gy'), may hold values from -1 to 1, as said below
Outputs:
- gauge_field: float32 [2, 3, 3, 4, 4, 2304], P(None, None, None, 'ta', 'gx', 'gy')
- time_rotated: float32 [2, 3, 3, 4, 4, 2304], P(None, None, None, 'ta', 'gx', 'gy')
- functional: float32 [4, 4], P(None, 'ta')
- theta: float32 [4], P('ta')
The draws below stay inside these ranges and needn't reach their ends.
Inputs may be any that keep to these rules, and one draw needn't show every extreme that they name: `space_links`: at every site the matrix is special unitary. `time_links`: at every site the matrix is special unitary. `start_gauge`: at every site the matrix is special unitary.
All inputs are finite; a program needn't handle non-finite values.
Results may differ from the reference program's by a relative error of at most 0.00021.
Values sent between devices are 32-bit elements; how exact they have to be, the bound alone decides.
No kernel may reach another device: no remote copies, remote signals or barrier semaphores. Data moves between devices by JAX's collectives and lax.ppermute only.
A program may use at most 64 MiB of HBM per device.

```python
import jax
import jax.numpy as jnp
from jax import lax

NZ = 48
ITERS = 4
NT = 4
NX = 4
NY = 48


PAIRS = ((0, 1), (1, 2), (0, 2))


SMALL = 1e-12


def turn_rows(matrix, row_one, row_two, coeffs):
    first_re, first_im = (matrix[0, row_one], matrix[1, row_one])
    second_re, second_im = (matrix[0, row_two], matrix[1, row_two])

    def scaled(real_part, imag_part, vec_re, vec_im):
        return (real_part * vec_re - imag_part * vec_im, real_part * vec_im + imag_part * vec_re)
    one_a = scaled(coeffs[0], coeffs[3], first_re, first_im)
    one_b = scaled(coeffs[2], coeffs[1], second_re, second_im)
    two_a = scaled(-coeffs[2], coeffs[1], first_re, first_im)
    two_b = scaled(coeffs[0], -coeffs[3], second_re, second_im)
    real_new = matrix[0].at[row_one].set(one_a[0] + one_b[0]).at[row_two].set(two_a[0] + two_b[0])
    imag_new = matrix[1].at[row_one].set(one_a[1] + one_b[1]).at[row_two].set(two_a[1] + two_b[1])
    return jnp.stack([real_new, imag_new])


def unitary_near(key, site_shape, spread):
    identity = jnp.eye(3, dtype=jnp.float32).reshape((3, 3) + (1,) * len(site_shape))
    real_part = jnp.broadcast_to(identity, (3, 3) + site_shape)
    matrix = jnp.stack([real_part, jnp.zeros_like(real_part)])
    for number in range(6):
        row_one, row_two = PAIRS[number % 3]
        noise = jax.random.normal(jax.random.fold_in(key, number), (4,) + site_shape, jnp.float32)
        quaternion = [1.0 + spread * noise[0], spread * noise[1], spread * noise[2], spread * noise[3]]
        length = jnp.sqrt(quaternion[0] * quaternion[0] + quaternion[1] * quaternion[1] + quaternion[2] * quaternion[2] + quaternion[3] * quaternion[3] + SMALL)
        coeffs = [entry / length for entry in quaternion]
        matrix = turn_rows(matrix, row_one, row_two, coeffs)
    return matrix


def ramp(low_end, high_end, flipped):
    x_coord = jnp.arange(NX).astype(jnp.float32) / NX
    y_coord = (jnp.arange(NY * NZ) // NZ).astype(jnp.float32) / NY
    level = (x_coord[:, None] + y_coord[None, :]) / 2.0
    if flipped:
        level = 1.0 - level
    return low_end + (high_end - low_end) * level


def draw_space_links(key, part):
    spread = ramp(0.1, 1.1, False)
    field = unitary_near(jax.random.fold_in(key, 11), (3, NT, NX, NY * NZ), spread)
    return jnp.moveaxis(field, 3, 0)


def draw_time_links(key, part):
    spread = 0.8
    return unitary_near(jax.random.fold_in(key, 23), (NT, NX, NY * NZ), spread)


def draw_start_gauge(key, part):
    spread = ramp(0.1, 1.6, True)
    return unitary_near(jax.random.fold_in(key, 37), (NT, NX, NY * NZ), spread)


def setup_inputs(seed: int = 0) -> dict:
    arg_keys = jax.random.split(jax.random.key(seed), 4)
    space_links = draw_space_links(jax.random.fold_in(arg_keys[3], 71), 0)
    time_links = draw_time_links(jax.random.fold_in(arg_keys[3], 71), 0)
    start_gauge = draw_start_gauge(jax.random.fold_in(arg_keys[3], 71), 0)
    return {"space_links": space_links, "time_links": time_links, "start_gauge": start_gauge}


OMEGA = 1.7
FLOOR = 0.5
PAIRS = ((0, 1), (1, 2), (0, 2))

def multiply(first, second):
    return lax.optimization_barrier(jnp.sum(first[:, :, None] * second[None, :, :], axis=1))

def product(left, right):
    return jnp.stack([multiply(left[0], right[0]) - multiply(left[1], right[1]), multiply(left[0], right[1]) + multiply(left[1], right[0])])

def dagger(matrix):
    return jnp.stack([jnp.swapaxes(matrix[0], 0, 1), -jnp.swapaxes(matrix[1], 0, 1)])

def z_ahead(field, z_index):
    return jnp.where(z_index == NZ - 1, jnp.roll(field, NZ - 1, axis=-1), jnp.roll(field, -1, axis=-1))

def z_behind(field, z_index):
    return jnp.where(z_index == 0, jnp.roll(field, -(NZ - 1), axis=-1), jnp.roll(field, 1, axis=-1))

def staples(links_now, back_links, forward, backward):
    staple_sum = jnp.zeros_like(forward[0])
    for direction in range(3):
        staple_sum = staple_sum + product(links_now[direction], dagger(forward[direction]))
        staple_sum = staple_sum + product(back_links[direction], dagger(backward[direction]))
    return staple_sum

def rotate_rows(matrix, row_one, row_two, coeffs):
    first_re, first_im = (matrix[0, row_one], matrix[1, row_one])
    second_re, second_im = (matrix[0, row_two], matrix[1, row_two])

    def scaled(real_part, imag_part, vec_re, vec_im):
        return (real_part * vec_re - imag_part * vec_im, real_part * vec_im + imag_part * vec_re)
    one_a = scaled(coeffs[0], coeffs[3], first_re, first_im)
    one_b = scaled(coeffs[2], coeffs[1], second_re, second_im)
    two_a = scaled(-coeffs[2], coeffs[1], first_re, first_im)
    two_b = scaled(coeffs[0], -coeffs[3], second_re, second_im)
    real_new = matrix[0].at[row_one].set(one_a[0] + one_b[0]).at[row_two].set(two_a[0] + two_b[0])
    imag_new = matrix[1].at[row_one].set(one_a[1] + one_b[1]).at[row_two].set(two_a[1] + two_b[1])
    return jnp.stack([real_new, imag_new])

def relax_sites(gauge_field, staple_sum, chosen):
    moment = product(gauge_field, staple_sum)
    candidate = gauge_field
    for row_one, row_two in PAIRS:
        vector = [moment[0, row_one, row_one] + moment[0, row_two, row_two], -(moment[1, row_one, row_two] + moment[1, row_two, row_one]), moment[0, row_two, row_one] - moment[0, row_one, row_two], moment[1, row_two, row_two] - moment[1, row_one, row_one]]
        length = jnp.sqrt(vector[0] * vector[0] + vector[1] * vector[1] + vector[2] * vector[2] + vector[3] * vector[3])
        pushed = [(1.0 - OMEGA) * length + OMEGA * vector[0], OMEGA * vector[1], OMEGA * vector[2], OMEGA * vector[3]]
        inverse = 1.0 / jnp.maximum(jnp.sqrt(pushed[0] * pushed[0] + pushed[1] * pushed[1] + pushed[2] * pushed[2] + pushed[3] * pushed[3]), FLOOR)
        coeffs = [entry * inverse for entry in pushed]
        candidate = rotate_rows(candidate, row_one, row_two, coeffs)
        moment = rotate_rows(moment, row_one, row_two, coeffs)
    trace_re = moment[0, 0, 0] + moment[0, 1, 1] + moment[0, 2, 2]
    return (jnp.where(chosen, candidate, gauge_field), jnp.where(chosen, trace_re, 0.0))

def antihermitian(matrix):
    half = (matrix - dagger(matrix)) / 2.0
    trace_im = half[1, 0, 0] + half[1, 1, 1] + half[1, 2, 2]
    identity = jnp.eye(3, dtype=matrix.dtype).reshape((3, 3) + (1,) * (matrix.ndim - 3))
    return jnp.stack([half[0], half[1] - identity * (trace_im / 3.0)])

def divergence_squares(gauge_field, links_now, lower_links, forward, backward):
    delta = jnp.zeros_like(gauge_field)
    for direction in range(3):
        here = product(product(gauge_field, links_now[direction]), dagger(forward[direction]))
        there = product(product(backward[direction], lower_links[direction]), dagger(gauge_field))
        delta = delta + antihermitian(there) - antihermitian(here)
    return lax.optimization_barrier(jnp.sum(delta * delta, axis=(0, 1, 2)))

def reference(space_links, time_links, start_gauge):
    x_count = space_links.shape[-2]
    row_width = space_links.shape[-1]
    volume = x_count * row_width
    z_index = jnp.arange(row_width) % NZ
    parity = (jnp.arange(x_count)[:, None] + (jnp.arange(row_width) // NZ)[None, :] + z_index[None, :]) % 2

    def neighbours(gauge_field):
        forward = [jnp.roll(gauge_field, -1, axis=-2), jnp.roll(gauge_field, -NZ, axis=-1), z_ahead(gauge_field, z_index)]
        backward = [jnp.roll(gauge_field, 1, axis=-2), jnp.roll(gauge_field, NZ, axis=-1), z_behind(gauge_field, z_index)]
        return (forward, backward)

    def fix_slice(inputs):
        links_now, gauge_field = inputs
        lower_links = [jnp.roll(links_now[0], 1, axis=-2), jnp.roll(links_now[1], NZ, axis=-1), z_behind(links_now[2], z_index)]
        back_links = [dagger(lower_link) for lower_link in lower_links]
        scores = []
        for iteration in range(ITERS):
            for colour in (0, 1):
                forward, backward = neighbours(gauge_field)
                staple_sum = staples(links_now, back_links, forward, backward)
                gauge_field, local_terms = relax_sites(gauge_field, staple_sum, parity == colour)
            scores.append(jnp.sum(local_terms) / (9.0 * volume))
        forward, backward = neighbours(gauge_field)
        theta_value = jnp.sum(divergence_squares(gauge_field, links_now, lower_links, forward, backward)) / (3.0 * volume)
        return (gauge_field, jnp.stack(scores), theta_value)
    gauges, scores, theta = lax.map(fix_slice, (jnp.moveaxis(space_links, 4, 0), jnp.moveaxis(start_gauge, 3, 0)))
    following = jnp.roll(gauges, -1, axis=0)

    def rotate_time(inputs):
        here, link_now, ahead_gauge = inputs
        return product(product(here, link_now), dagger(ahead_gauge))
    rotated = lax.map(rotate_time, (gauges, jnp.moveaxis(time_links, 3, 0), following))
    return (jnp.moveaxis(gauges, 0, 3), jnp.moveaxis(rotated, 0, 3), jnp.transpose(scores), theta)
```

```python
import math

import jax
import jax.numpy as jnp
from jax import lax
from jax.experimental import pallas as pl
from jax.experimental.pallas import tpu as pltpu
from jax.sharding import PartitionSpec as P

NZ = 48
ITERS = 4

OMEGA = 1.7
FLOOR = 0.5
PAIRS = ((0, 1), (1, 2), (0, 2))

LANES = 128
HALF = LANES // 2
BLOCK_ROWS = LANES // math.gcd(NZ, LANES)
TILES = BLOCK_ROWS * NZ // LANES
BLOCK = BLOCK_ROWS * NZ
WINDOW = 4
LINK_PARTS = 36
PARTS = 48
GAUGE_AT = LINK_PARTS
ROW_Y = 12


def part_index(part):
    matrix, rest = divmod(part, 12)
    reim, rest = divmod(rest, 6)
    return matrix, reim * 9 + rest


def pack_kernel(own_tiles, links, gauge, own, below, above):
    width = gauge.shape[-1]
    lane = lax.broadcasted_iota(jnp.int32, (2, width), 1)
    odd = (lane // NZ + lane % NZ) % 2 == 1
    low = lax.broadcasted_iota(jnp.int32, (2, LANES), 1) < HALF
    extra_below = 0
    extra_above = 0
    for part in range(PARTS):
        matrix, entry = part_index(part)
        both = links[matrix * 18 + entry] if matrix < 3 else gauge[entry]
        swapped = jnp.concatenate([both[1:2], both[0:1]], axis=0)
        packed = jnp.where(odd, swapped, both)
        last = width - (own_tiles - 1) * LANES
        tiles = [packed[:, t * LANES : (t + 1) * LANES] for t in range(own_tiles - 1)]
        tiles.append(
            jnp.concatenate(
                [packed[:, width - last :], jnp.zeros((2, LANES - last), jnp.float32)], axis=1
            )
        )
        turned = [pltpu.roll(tile, HALF, 1) for tile in tiles]
        for t in range(own_tiles):
            shifted = jnp.where(low, turned[t - 1] if t else turned[0], turned[t])
            own[pl.ds((part * own_tiles + t) * 2, 2), :] = shifted
        first = own_tiles - 1 - TILES
        edge = jnp.where(low, tiles[own_tiles - 1], tiles[first])
        for t in range(TILES):
            body = edge if t == 0 else tiles[first + t]
            below[pl.ds((part * TILES + t) * 2, 2), :] = body
            above[pl.ds((part * TILES + t) * 2, 2), :] = tiles[t]
        if ROW_Y <= part < ROW_Y + 12 or part >= GAUGE_AT:
            below[pl.ds(PARTS * TILES * 2 + extra_below, 1), :] = tiles[first][1:2]
            extra_below += 1
        if part >= GAUGE_AT:
            above[pl.ds(PARTS * TILES * 2 + extra_above, 1), :] = tiles[TILES][1:2]
            extra_above += 1
    rest = above.shape[0] - (PARTS * TILES * 2 + extra_above)
    above[pl.ds(above.shape[0] - rest, rest), :] = jnp.zeros((rest, LANES), jnp.float32)


def pack(links, gauge):
    width = gauge.shape[-1]
    own_tiles = -(-width // LANES)
    rows = PARTS * TILES * 2
    shapes = [
        jax.ShapeDtypeStruct((PARTS * own_tiles * 2, LANES), jnp.float32),
        jax.ShapeDtypeStruct((rows + 24, LANES), jnp.float32),
        jax.ShapeDtypeStruct((rows + 16, LANES), jnp.float32),
    ]
    return pl.pallas_call(
        lambda *refs: pack_kernel(own_tiles, *refs),
        out_shape=shapes,
        name="pack",
    )(links, gauge)


def row_roll(value, shift):
    return pltpu.roll(value, shift % value.shape[0], 0)


def lane_roll(value, shift):
    return pltpu.roll(value, shift % LANES, 1)


class Masks:
    def __init__(self, rows):
        self.rows = rows
        self.lane = lax.broadcasted_iota(jnp.int32, (rows, LANES), 1)
        self.block = lax.broadcasted_iota(jnp.int32, (rows, LANES), 0) % WINDOW

    def z(self, tile):
        return (self.lane + tile * LANES) % NZ

    def odd(self, tile):
        return ((self.lane + tile * LANES) // NZ + self.z(tile)) % 2 == 1

    def owned(self, tile, start, width):
        place = self.block * BLOCK + tile * LANES + self.lane
        return (place >= start) & (place < start + width)


def y_ahead(tiles, masks):
    turned = [lane_roll(tile, -NZ) for tile in tiles]
    turned.append(row_roll(turned[0], -1))
    inside = masks.lane < LANES - NZ
    return [jnp.where(inside, turned[j], turned[j + 1]) for j in range(TILES)]


def y_behind(tiles, masks):
    turned = [lane_roll(tile, NZ) for tile in tiles]
    before = row_roll(turned[TILES - 1], 1)
    inside = masks.lane >= NZ
    return [jnp.where(inside, turned[j], turned[j - 1] if j else before) for j in range(TILES)]


def z_ahead(tiles, masks):
    step = [lane_roll(tile, -1) for tile in tiles]
    wrap = [lane_roll(tile, NZ - 1) for tile in tiles]
    out = []
    for j in range(TILES):
        near = step[j]
        if j < TILES - 1:
            near = jnp.where(masks.lane < LANES - 1, step[j], step[j + 1])
        far = wrap[j]
        if j:
            far = jnp.where(masks.lane >= NZ - 1, wrap[j], wrap[j - 1])
        out.append(jnp.where(masks.z(j) == NZ - 1, far, near))
    return out


def z_behind(tiles, masks):
    step = [lane_roll(tile, 1) for tile in tiles]
    wrap = [lane_roll(tile, 1 - NZ) for tile in tiles]
    out = []
    for j in range(TILES):
        near = step[j]
        if j:
            near = jnp.where(masks.lane >= 1, step[j], step[j - 1])
        far = wrap[j]
        if j < TILES - 1:
            far = jnp.where(masks.lane < LANES - NZ + 1, wrap[j], wrap[j + 1])
        out.append(jnp.where(masks.z(j) == 0, far, near))
    return out


def tile_of(j):
    return slice(j * LANES, (j + 1) * LANES)


def times_dagger(total, left, right):
    left_re, left_im = left
    right_re, right_im = right
    out_re = []
    out_im = []
    for a in range(3):
        for b in range(3):
            re = None if total is None else total[0][3 * a + b]
            im = None if total is None else total[1][3 * a + b]
            for c in range(3):
                lr, li = left_re[3 * a + c], left_im[3 * a + c]
                rr, ri = right_re[3 * b + c], right_im[3 * b + c]
                term = lr * rr
                re = term if re is None else re + term
                re = re + li * ri
                term = li * rr
                im = term if im is None else im + term
                im = im - lr * ri
            out_re.append(re)
            out_im.append(im)
    return out_re, out_im


def times(left, right):
    left_re, left_im = left
    right_re, right_im = right
    out_re = []
    out_im = []
    for a in range(3):
        for b in range(3):
            re = im = None
            for c in range(3):
                lr, li = left_re[3 * a + c], left_im[3 * a + c]
                rr, ri = right_re[3 * c + b], right_im[3 * c + b]
                re = lr * rr if re is None else re + lr * rr
                re = re - li * ri
                im = lr * ri if im is None else im + lr * ri
                im = im + li * rr
            out_re.append(re)
            out_im.append(im)
    return out_re, out_im


def relax_coeffs(moment, one, two):
    re, im = moment
    c0 = re[4 * one] + re[4 * two]
    c1 = -(im[3 * one + two] + im[3 * two + one])
    c2 = re[3 * two + one] - re[3 * one + two]
    c3 = im[4 * two] - im[4 * one]
    length = jnp.sqrt(c0 * c0 + c1 * c1 + c2 * c2 + c3 * c3)
    v0 = (1.0 - OMEGA) * length + OMEGA * c0
    v1 = OMEGA * c1
    v2 = OMEGA * c2
    v3 = OMEGA * c3
    scale = lax.rsqrt(jnp.maximum(v0 * v0 + v1 * v1 + v2 * v2 + v3 * v3, FLOOR * FLOOR))
    return v0 * scale, v1 * scale, v2 * scale, v3 * scale


def turn_rows(matrix, one, two, coeffs):
    a0, a1, a2, a3 = coeffs
    re = list(matrix[0])
    im = list(matrix[1])
    for col in range(3):
        f, s = 3 * one + col, 3 * two + col
        fr, fi, sr, si = re[f], im[f], re[s], im[s]
        re[f] = (a0 * fr - a3 * fi) + (a2 * sr - a1 * si)
        im[f] = (a0 * fi + a3 * fr) + (a2 * si + a1 * sr)
        re[s] = (a0 * sr + a3 * si) - (a2 * fr + a1 * fi)
        im[s] = (a0 * si - a3 * sr) + (a1 * fr - a2 * fi)
    return re, im


def antihermitian_squares(moment):
    re, im = moment
    total = None
    for a, b in PAIRS:
        dr = re[3 * a + b] - re[3 * b + a]
        di = im[3 * a + b] + im[3 * b + a]
        term = dr * dr + di * di
        total = term if total is None else total + term
    third = (im[0] + im[4] + im[8]) * (1.0 / 3.0)
    total = 0.5 * total
    for a in range(3):
        part = im[4 * a] - third
        total = total + part * part
    return total


def sweep_kernel(pairs, own_tiles, width, *refs):
    own = refs[0:pairs]
    below = refs[pairs : 2 * pairs]
    above = refs[2 * pairs : 3 * pairs]
    gauge_out, sums_out = refs[3 * pairs : 3 * pairs + 2]
    flat, extra, link, staple_link, field, moved, scores = refs[3 * pairs + 2 :]
    rows = pairs * WINDOW
    per_pair = WINDOW * TILES
    stride = pairs * per_pair
    start = WINDOW * BLOCK - width - (WINDOW * BLOCK - 2 * width)
    first_own = start // LANES
    masks = Masks(rows)

    for part in range(PARTS):
        for colour in range(2):
            for p in range(pairs):
                base = (colour * PARTS + part) * stride + p * per_pair
                flat[pl.ds(base + 1, TILES), :] = below[p][
                    pl.ds(part * TILES * 2 + colour, TILES, stride=2), :
                ]
                flat[pl.ds(base + first_own, own_tiles), :] = own[p][
                    pl.ds(part * own_tiles * 2 + colour, own_tiles, stride=2), :
                ]
                flat[pl.ds(base + per_pair - TILES, TILES), :] = above[p][
                    pl.ds(part * TILES * 2 + colour, TILES, stride=2), :
                ]
    for p in range(pairs):
        for i in range(24):
            extra[pl.ds(i * rows + WINDOW * p, 1), :] = below[p][pl.ds(PARTS * TILES * 2 + i, 1), :]
        for i in range(12):
            ahead = WINDOW * ((p + 1) % pairs)
            extra[pl.ds((24 + i) * rows + ahead, 1), :] = above[p][
                pl.ds(PARTS * TILES * 2 + i, 1), :
            ]

    first_block = masks.block == 0
    low_lanes = masks.lane < HALF
    low_second = (masks.block == 1) & low_lanes
    low_first = first_block & low_lanes

    def loaded(colour, part, j):
        base = (colour * PARTS + part) * stride
        value = flat[pl.ds(base + j, rows, stride=TILES), :]
        edge_y = ROW_Y <= part < ROW_Y + 12
        edge_g = part >= GAUGE_AT
        if j == 0:
            fill = jnp.zeros_like(value)
            if colour == 1 and edge_g:
                fill = extra[pl.ds((24 + part - GAUGE_AT) * rows, rows), :]
            value = jnp.where(first_block, fill, value)
        if j == 1:
            value = jnp.where(low_second, row_roll(value, 1), value)
            if colour == 1 and (edge_y or edge_g):
                at = part - ROW_Y if edge_y else 12 + part - GAUGE_AT
                value = jnp.where(low_first, extra[pl.ds(at * rows, rows), :], value)
        return value

    for colour in range(2):
        for matrix in range(4):
            target = link if matrix < 3 else field
            at = (colour * 3 + matrix) * 18 if matrix < 3 else colour * 18
            for j in range(TILES):
                parts = [loaded(colour, matrix * 12 + i, j) for i in range(12)]
                ar, br = parts[0:3], parts[3:6]
                ai, bi = parts[6:9], parts[9:12]
                for i in range(3):
                    target[at + i, :, tile_of(j)] = ar[i]
                    target[at + 3 + i, :, tile_of(j)] = br[i]
                    target[at + 9 + i, :, tile_of(j)] = ai[i]
                    target[at + 12 + i, :, tile_of(j)] = bi[i]
                    k, n = (i + 1) % 3, (i + 2) % 3
                    third_re = (ar[k] * br[n] - ai[k] * bi[n]) - (ar[n] * br[k] - ai[n] * bi[k])
                    third_im = (ar[n] * bi[k] + ai[n] * br[k]) - (ar[k] * bi[n] + ai[k] * br[n])
                    target[at + 6 + i, :, tile_of(j)] = third_re
                    target[at + 15 + i, :, tile_of(j)] = third_im

    def read(ref, at):
        return [ref[at, :, tile_of(j)] for j in range(TILES)]

    def write(ref, at, tiles):
        for j in range(TILES):
            ref[at, :, tile_of(j)] = tiles[j]

    for colour in range(2):
        for reim in range(2):
            for a in range(3):
                for c in range(3):
                    here = reim * 9 + 3 * a + c
                    there = reim * 9 + 3 * c + a
                    sign = -1.0 if reim else 1.0
                    ours = read(link, (colour * 3) * 18 + here)
                    theirs = [sign * t for t in read(link, ((1 - colour) * 3) * 18 + there)]
                    behind = [row_roll(t, WINDOW) for t in theirs]
                    same = []
                    other = []
                    for j in range(TILES):
                        lower = masks.odd(j) if colour else ~masks.odd(j)
                        same.append(jnp.where(lower, ours[j], theirs[j]))
                        other.append(jnp.where(lower, behind[j], ours[j]))
                    write(staple_link, (colour * 4 + 0) * 18 + here, same)
                    write(staple_link, (colour * 4 + 1) * 18 + here, other)
                    theirs = [sign * t for t in read(link, ((1 - colour) * 3 + 1) * 18 + there)]
                    write(staple_link, (colour * 4 + 2) * 18 + here, y_behind(theirs, masks))
                    theirs = [sign * t for t in read(link, ((1 - colour) * 3 + 2) * 18 + there)]
                    write(staple_link, (colour * 4 + 3) * 18 + here, z_behind(theirs, masks))

    def move(colour):
        for i in range(18):
            tiles = read(field, colour * 18 + i)
            behind = [row_roll(t, WINDOW) for t in tiles]
            if 2 * WINDOW == rows:
                other = behind
            else:
                other = []
                for j in range(TILES):
                    lower = ~masks.odd(j) if colour else masks.odd(j)
                    other.append(jnp.where(lower, behind[j], row_roll(tiles[j], -WINDOW)))
            at = colour * 5 * 18 + i
            write(moved, at, other)
            write(moved, at + 18, y_ahead(tiles, masks))
            write(moved, at + 36, y_behind(tiles, masks))
            write(moved, at + 54, z_ahead(tiles, masks))
            write(moved, at + 72, z_behind(tiles, masks))

    def matrix_at(ref, at, group, j):
        block = [ref[at + i, group, tile_of(j)] for i in range(18)]
        return block[:9], block[9:]

    def moment_of(colour, group, j):
        them = 1 - colour
        total = None
        links = (
            (staple_link, (colour * 4 + 0) * 18),
            (staple_link, (colour * 4 + 1) * 18),
            (link, (colour * 3 + 1) * 18),
            (staple_link, (colour * 4 + 2) * 18),
            (link, (colour * 3 + 2) * 18),
            (staple_link, (colour * 4 + 3) * 18),
        )
        for number, (ref, at) in enumerate(links):
            if number == 0:
                right = matrix_at(field, them * 18, group, j)
            else:
                right = matrix_at(moved, (them * 5 + number - 1) * 18, group, j)
            total = times_dagger(total, matrix_at(ref, at, group, j), right)
        gauge = matrix_at(field, colour * 18, group, j)
        return gauge, times(gauge, total)

    def groups(body, init):
        count = rows // 8
        if count == 1:
            return body(0, pl.ds(0, 8), init)
        return lax.fori_loop(
            0, count, lambda g, carry: body(g, pl.ds(pl.multiple_of(g * 8, 8), 8), carry), init
        )

    group_masks = Masks(8)
    owned = [group_masks.owned(j, start, width) for j in range(TILES)]
    zero = jnp.zeros((8, LANES), jnp.float32)

    def half_sweep(colour):
        def body(g, group, carry):
            score, squares = carry
            for j in range(TILES):
                gauge, moment = moment_of(colour, group, j)
                for one, two in PAIRS:
                    coeffs = relax_coeffs(moment, one, two)
                    gauge = turn_rows(gauge, one, two, coeffs)
                    moment = turn_rows(moment, one, two, coeffs)
                for i in range(9):
                    field[colour * 18 + i, group, tile_of(j)] = gauge[0][i]
                    field[colour * 18 + 9 + i, group, tile_of(j)] = gauge[1][i]
                if colour == 1:
                    trace = moment[0][0] + moment[0][4] + moment[0][8]
                    score = score + jnp.where(owned[j], trace, 0.0)
                    squares = squares + jnp.where(owned[j], antihermitian_squares(moment), 0.0)
            return score, squares

        return groups(body, (zero, zero))

    move(1)

    def iteration(k, carry):
        half_sweep(0)
        move(0)
        score, squares = half_sweep(1)
        move(1)
        scores[k] = score
        scores[ITERS] = squares
        return carry

    lax.fori_loop(0, ITERS, iteration, 0)

    def theta_body(g, group, squares):
        for j in range(TILES):
            _, moment = moment_of(0, group, j)
            squares = squares + jnp.where(owned[j], antihermitian_squares(moment), 0.0)
        return squares

    scores[ITERS] = groups(theta_body, scores[ITERS])

    line = lax.broadcasted_iota(jnp.int32, (8, LANES), 0)
    sums = zero
    for k in range(ITERS + 1):
        sums = jnp.where(line == k, jnp.sum(scores[k]), sums)
    sums_out[...] = sums

    tile_line = lax.broadcasted_iota(jnp.int32, (own_tiles, LANES), 0)
    tile_lane = lax.broadcasted_iota(jnp.int32, (own_tiles, LANES), 1)
    place = tile_line * LANES + tile_lane
    odd = (place // NZ + place % NZ) % 2 == 1
    low = tile_lane < HALF
    for i in range(18):
        colours = []
        for colour in range(2):
            base = (colour * PARTS + i) * stride
            for j in range(TILES):
                flat[pl.ds(base + j, rows, stride=TILES), :] = field[colour * 18 + i, :, tile_of(j)]
            early = flat[pl.ds(base + first_own, own_tiles), :]
            late = flat[pl.ds(base + first_own + 1, own_tiles), :]
            colours.append(jnp.where(low, lane_roll(early, HALF), lane_roll(late, HALF)))
        planes = (
            jnp.where(odd, colours[1], colours[0]),
            jnp.where(odd, colours[0], colours[1]),
        )
        for x in range(2):
            for t in range(own_tiles):
                size = min(LANES, width - t * LANES)
                gauge_out[i, x : x + 1, t * LANES : t * LANES + size] = planes[x][
                    t : t + 1, :size
                ]


def sweeps(own, below, above, width):
    pairs = len(own)
    own_tiles = -(-width // LANES)
    rows = pairs * WINDOW
    stride = pairs * WINDOW * TILES
    cells = lambda count: pltpu.VMEM((count, rows, BLOCK), jnp.float32)
    return pl.pallas_call(
        lambda *refs: sweep_kernel(pairs, own_tiles, width, *refs),
        out_shape=[
            jax.ShapeDtypeStruct((18, 2, width), jnp.float32),
            jax.ShapeDtypeStruct((8, LANES), jnp.float32),
        ],
        scratch_shapes=[
            pltpu.VMEM((2 * PARTS * stride, LANES), jnp.float32),
            pltpu.VMEM((36 * rows, LANES), jnp.float32),
            cells(2 * 3 * 18),
            cells(2 * 4 * 18),
            cells(2 * 18),
            cells(2 * 5 * 18),
            pltpu.VMEM((8, 8, LANES), jnp.float32),
        ],
        compiler_params=pltpu.CompilerParams(vmem_limit_bytes=56 * 1024 * 1024),
        name="sweeps",
    )(*own, *below, *above)


def rotate_kernel(here, links, ahead, out):
    def matrix(ref):
        return [ref[i] for i in range(9)], [ref[9 + i] for i in range(9)]

    re, im = times_dagger(None, times(matrix(here), matrix(links)), matrix(ahead))
    for i in range(9):
        out[i] = re[i]
        out[9 + i] = im[i]


def rotate(here, links, ahead):
    return pl.pallas_call(
        rotate_kernel, out_shape=jax.ShapeDtypeStruct(here.shape, here.dtype), name="rotate"
    )(here, links, ahead)


def from_ahead(block, axis, distance):
    count = lax.axis_size(axis)
    return lax.ppermute(block, axis, [((i + distance) % count, i) for i in range(count)])


def local(space_links, time_links, start_gauge):
    x_sites, width = start_gauge.shape[-2:]
    pairs = lax.axis_size("gx")
    volume = x_sites * pairs * width * lax.axis_size("gy")
    assert x_sites == 2 and start_gauge.shape[3] == 1
    assert width % NZ == 0 and (width // NZ) % 2 == 0 and width % LANES == HALF
    assert 2 * width + BLOCK == WINDOW * BLOCK and pairs >= 2
    assert BLOCK_ROWS >= 2 * ITERS

    own, below, above = pack(
        space_links.reshape(54, x_sites, width), start_gauge.reshape(18, x_sites, width)
    )
    below = from_ahead(below, "gy", -1)
    above = from_ahead(above, "gy", 1)
    owns = [own] + [from_ahead(own, "gx", i) for i in range(1, pairs)]
    belows = [below] + [from_ahead(below, "gx", i) for i in range(1, pairs)]
    aboves = [above] + [from_ahead(above, "gx", i) for i in range(1, pairs)]
    gauge, sums = sweeps(owns, belows, aboves, width)
    ahead = from_ahead(gauge, "ta", 1)
    count = lax.axis_size("gy")
    step = 1
    if count & (count - 1) == 0:
        while step < count:
            sums = sums + lax.ppermute(sums, "gy", [(i, i ^ step) for i in range(count)])
            step *= 2
    else:
        sums = sums + sum(from_ahead(sums, "gy", i) for i in range(1, count))
    rotated = rotate(gauge, time_links.reshape(18, x_sites, width), ahead)
    functional = sums[:ITERS, :1] / (9.0 * volume)
    theta = sums[ITERS, :1] / (3.0 * volume)
    return (gauge.reshape(start_gauge.shape), rotated.reshape(start_gauge.shape), functional, theta)


def solution(mesh):
    placed = (
        P(None, None, None, None, "ta", "gx", "gy"),
        P(None, None, None, "ta", "gx", "gy"),
        P(None, None, None, "ta", "gx", "gy"),
    )
    return jax.shard_map(
        local,
        mesh=mesh,
        in_specs=placed,
        out_specs=(
            P(None, None, None, "ta", "gx", "gy"),
            P(None, None, None, "ta", "gx", "gy"),
            P(None, "ta"),
            P("ta"),
        ),
        check_vma=False,
    )
```

```python
import math

import jax
import jax.numpy as jnp
from jax import lax
from jax.experimental import pallas as pl
from jax.experimental.pallas import tpu as pltpu
from jax.sharding import PartitionSpec as P


NZ = 48
ITERS = 4

OMEGA = 1.7
FLOOR = 0.5
PAIRS = ((0, 1), (1, 2), (0, 2))

LANES = 128
HALF = LANES // 2
BLOCK_ROWS = LANES // math.gcd(NZ, LANES)
TILES = BLOCK_ROWS * NZ // LANES
BLOCK = BLOCK_ROWS * NZ
WINDOW = 4
COORDS = 8
PARTS = 4 * COORDS
ROW_Y = COORDS
GAUGE_AT = 3 * COORDS
POLE = 1e15
NEAR_POLE = 1e-30


def to_plane(point):
    first, rest = point[0], point[1:]
    square = rest[0] * rest[0]
    for entry in rest[1:]:
        square = square + entry * entry
    upper = first >= 0.0
    top = jnp.where(upper, 1.0, 1.0 - first)
    bottom = jnp.where(upper, 1.0 + first, jnp.maximum(square, NEAR_POLE))
    scale = top / bottom
    plane = [scale * entry for entry in rest]
    at_pole = (first < 0.0) & (square < NEAR_POLE)
    plane[0] = jnp.where(at_pole, POLE, plane[0])
    return plane


def from_plane(plane):
    square = plane[0] * plane[0]
    for entry in plane[1:]:
        square = square + entry * entry
    scale = 2.0 / (1.0 + square)
    return scale, [scale - 1.0] + [scale * entry for entry in plane]


def row_and_basis(plane):
    scale, point = from_plane(plane)
    row = [(point[0], point[1]), (point[2], point[3]), (point[4], point[5])]
    u = [(scale, point[1]), row[1], row[2]]
    tilt = plane[0]
    inverse = 1.0 / (1.0 + tilt * tilt)
    basis = []
    for j in (1, 2):
        re, im = plane[2 * j - 1], plane[2 * j]
        zr = (re + im * tilt) * inverse
        zi = (re * tilt - im) * inverse
        vector = []
        for k in range(3):
            ur, ui = u[k]
            br = ui * zi - ur * zr
            bi = -(ur * zi + ui * zr)
            vector.append((1.0 + br, bi) if k == j else (br, bi))
        basis.append(vector)
    return row, basis


def encode(first, second):
    point = [part for entry in first for part in entry]
    plane = to_plane(point)
    _, basis = row_and_basis(plane)
    coeffs = []
    for vector in basis:
        re = im = None
        for (sr, si), (br, bi) in zip(second, vector):
            tr = sr * br + si * bi
            ti = si * br - sr * bi
            re = tr if re is None else re + tr
            im = ti if im is None else im + ti
        coeffs += [re, im]
    return plane + to_plane(coeffs)


def decode(coords):
    first, basis = row_and_basis(coords[:5])
    _, coeffs = from_plane(coords[5:])
    second = []
    for k in range(3):
        re = im = None
        for j in range(2):
            cr, ci = coeffs[2 * j], coeffs[2 * j + 1]
            br, bi = basis[j][k]
            tr = cr * br - ci * bi
            ti = cr * bi + ci * br
            re = tr if re is None else re + tr
            im = ti if im is None else im + ti
        second.append((re, im))
    third = []
    for i in range(3):
        (ar, ai), (cr, ci) = first[(i + 1) % 3], first[(i + 2) % 3]
        (br, bi), (dr, di) = second[(i + 1) % 3], second[(i + 2) % 3]
        re = (ar * dr - ai * di) - (cr * br - ci * bi)
        im = (cr * bi + ci * br) - (ar * di + ai * dr)
        third.append((re, im))
    rows = first + second + third
    return [entry[0] for entry in rows], [entry[1] for entry in rows]


def pack_kernel(
    own_tiles, links_hbm, gauge_hbm, own, below, above, links, gauge, natural, coded, arrived
):
    copies = [pltpu.make_async_copy(gauge_hbm, gauge, arrived.at[0])]
    copies.append(pltpu.make_async_copy(links_hbm, links, arrived.at[1]))
    for copy in copies:
        copy.start()
    for copy in copies:
        copy.wait()
    width = gauge.shape[-1]
    last = width - (own_tiles - 1) * LANES
    lane = lax.broadcasted_iota(jnp.int32, (2, width), 1)
    odd = (lane // NZ + lane % NZ) % 2 == 1
    rows = 2 * own_tiles
    for matrix in (3, 0, 1, 2):
        for number in range(12):
            entry = number if number < 6 else number + 3
            both = gauge[entry] if matrix == 3 else links[matrix * 18 + entry]
            swapped = jnp.concatenate([both[1:2], both[0:1]], axis=0)
            packed = jnp.where(odd, swapped, both)
            for t in range(own_tiles):
                tile = packed[:, t * LANES : (t + 1) * LANES]
                if t == own_tiles - 1:
                    tile = jnp.concatenate([tile, jnp.zeros((2, LANES - last), jnp.float32)], axis=1)
                natural[pl.ds((matrix * 12 + number) * rows + 2 * t, 2), :] = tile
        values = [natural[pl.ds((matrix * 12 + i) * rows, rows), :] for i in range(12)]
        entries = [(values[i], values[6 + i]) for i in range(6)]
        for i, value in enumerate(encode(entries[:3], entries[3:])):
            coded[pl.ds(8 + (matrix * COORDS + i) * rows, rows), :] = value
    low = lax.broadcasted_iota(jnp.int32, (rows, LANES), 1) < HALF
    first = own_tiles - 1 - TILES
    extra_below = extra_above = PARTS * TILES * 2
    for part in range(PARTS):
        base = 8 + part * rows
        here = pltpu.roll(coded[pl.ds(base, rows), :], HALF, 1)
        before = pltpu.roll(coded[pl.ds(base - 2, rows), :], HALF, 1)
        own[pl.ds(part * rows, rows), :] = jnp.where(low, before, here)
        at = part * TILES * 2
        edge = jnp.where(
            low[:2],
            coded[pl.ds(base + 2 * (own_tiles - 1), 2), :],
            coded[pl.ds(base + 2 * first, 2), :],
        )
        below[pl.ds(at, 2), :] = edge
        below[pl.ds(at + 2, 2 * TILES - 2), :] = coded[
            pl.ds(base + 2 * first + 2, 2 * TILES - 2), :
        ]
        above[pl.ds(at, 2 * TILES), :] = coded[pl.ds(base, 2 * TILES), :]
        if ROW_Y <= part < ROW_Y + COORDS or part >= GAUGE_AT:
            below[pl.ds(extra_below, 1), :] = coded[pl.ds(base + 2 * first + 1, 1), :]
            extra_below += 1
        if part >= GAUGE_AT:
            above[pl.ds(extra_above, 1), :] = coded[pl.ds(base + 2 * TILES + 1, 1), :]
            extra_above += 1


def pack(links, gauge):
    width = gauge.shape[-1]
    own_tiles = -(-width // LANES)
    rows = PARTS * TILES * 2
    shapes = [
        jax.ShapeDtypeStruct((PARTS * own_tiles * 2, LANES), jnp.float32),
        jax.ShapeDtypeStruct((rows + 2 * COORDS, LANES), jnp.float32),
        jax.ShapeDtypeStruct((rows + COORDS, LANES), jnp.float32),
    ]
    return pl.pallas_call(
        lambda *refs: pack_kernel(own_tiles, *refs),
        out_shape=shapes,
        in_specs=[pl.BlockSpec(memory_space=pltpu.HBM)] * 2,
        scratch_shapes=[
            pltpu.VMEM(links.shape, links.dtype),
            pltpu.VMEM(gauge.shape, gauge.dtype),
            pltpu.VMEM((48 * own_tiles * 2, LANES), jnp.float32),
            pltpu.VMEM((8 + PARTS * own_tiles * 2, LANES), jnp.float32),
            pltpu.SemaphoreType.DMA((2,)),
        ],
        compiler_params=pltpu.CompilerParams(vmem_limit_bytes=6 << 20),
        name="pack",
    )(links, gauge)


def row_roll(value, shift):
    return pltpu.roll(value, shift % value.shape[0], 0)


def lane_roll(value, shift):
    return pltpu.roll(value, shift % LANES, 1)


class Masks:
    def __init__(self, rows):
        self.lane = lax.broadcasted_iota(jnp.int32, (rows, LANES), 1)
        self.block = lax.broadcasted_iota(jnp.int32, (rows, LANES), 0) % WINDOW

    def z(self, tile):
        return (self.lane + tile * LANES) % NZ

    def odd(self, tile):
        return ((self.lane + tile * LANES) // NZ + self.z(tile)) % 2 == 1

    def owned(self, tile, start, width):
        place = self.block * BLOCK + tile * LANES + self.lane
        return (place >= start) & (place < start + width)


def y_ahead(tiles, masks):
    turned = [lane_roll(tile, -NZ) for tile in tiles]
    turned.append(row_roll(turned[0], -1))
    inside = masks.lane < LANES - NZ
    return [jnp.where(inside, turned[j], turned[j + 1]) for j in range(TILES)]


def y_behind(tiles, masks):
    turned = [lane_roll(tile, NZ) for tile in tiles]
    before = row_roll(turned[TILES - 1], 1)
    inside = masks.lane >= NZ
    return [jnp.where(inside, turned[j], turned[j - 1] if j else before) for j in range(TILES)]


def z_ahead(tiles, masks):
    step = [lane_roll(tile, -1) for tile in tiles]
    wrap = [lane_roll(tile, NZ - 1) for tile in tiles]
    out = []
    for j in range(TILES):
        near = step[j]
        if j < TILES - 1:
            near = jnp.where(masks.lane < LANES - 1, step[j], step[j + 1])
        far = wrap[j]
        if j:
            far = jnp.where(masks.lane >= NZ - 1, wrap[j], wrap[j - 1])
        out.append(jnp.where(masks.z(j) == NZ - 1, far, near))
    return out


def z_behind(tiles, masks):
    step = [lane_roll(tile, 1) for tile in tiles]
    wrap = [lane_roll(tile, 1 - NZ) for tile in tiles]
    out = []
    for j in range(TILES):
        near = step[j]
        if j:
            near = jnp.where(masks.lane >= 1, step[j], step[j - 1])
        far = wrap[j]
        if j < TILES - 1:
            far = jnp.where(masks.lane < LANES - NZ + 1, wrap[j], wrap[j + 1])
        out.append(jnp.where(masks.z(j) == 0, far, near))
    return out


def tile_of(j):
    return slice(j * LANES, (j + 1) * LANES)


def times_dagger(left, right):
    left_re, left_im = left
    right_re, right_im = right
    out_re = []
    out_im = []
    for a in range(3):
        for b in range(3):
            re = im = None
            for c in range(3):
                lr, li = left_re[3 * a + c], left_im[3 * a + c]
                rr, ri = right_re[3 * b + c], right_im[3 * b + c]
                re = lr * rr if re is None else re + lr * rr
                re = re + li * ri
                im = li * rr if im is None else im + li * rr
                im = im - lr * ri
            out_re.append(re)
            out_im.append(im)
    return out_re, out_im


def add_staple(sums, link, gauge):
    gauge_re, gauge_im = gauge
    both = [gauge_re[i] + gauge_im[i] for i in range(9)]
    right = (both, gauge_im, gauge_re)
    out = []
    for k in range(3):
        entries = []
        for a in range(3):
            for b in range(3):
                value = None if sums is None else sums[k][3 * a + b]
                for c in range(3):
                    term = link[k][3 * a + c] * right[k][3 * b + c]
                    value = term if value is None else value + term
                entries.append(value)
        out.append(entries)
    return out


def times(left, right):
    left_re, left_im = left
    right_re, right_im = right
    out_re = []
    out_im = []
    for a in range(3):
        for b in range(3):
            re = im = None
            for c in range(3):
                lr, li = left_re[3 * a + c], left_im[3 * a + c]
                rr, ri = right_re[3 * c + b], right_im[3 * c + b]
                re = lr * rr if re is None else re + lr * rr
                re = re - li * ri
                im = lr * ri if im is None else im + lr * ri
                im = im + li * rr
            out_re.append(re)
            out_im.append(im)
    return out_re, out_im


def relax_coeffs(moment, one, two):
    re, im = moment
    c0 = re[4 * one] + re[4 * two]
    c1 = -(im[3 * one + two] + im[3 * two + one])
    c2 = re[3 * two + one] - re[3 * one + two]
    c3 = im[4 * two] - im[4 * one]
    length = jnp.sqrt(c0 * c0 + c1 * c1 + c2 * c2 + c3 * c3)
    v0 = (1.0 - OMEGA) * length + OMEGA * c0
    v1 = OMEGA * c1
    v2 = OMEGA * c2
    v3 = OMEGA * c3
    scale = lax.rsqrt(jnp.maximum(v0 * v0 + v1 * v1 + v2 * v2 + v3 * v3, FLOOR * FLOOR))
    return v0 * scale, v1 * scale, v2 * scale, v3 * scale


def turn_rows(matrix, one, two, coeffs):
    a0, a1, a2, a3 = coeffs
    re = list(matrix[0])
    im = list(matrix[1])
    for col in range(3):
        f, s = 3 * one + col, 3 * two + col
        fr, fi, sr, si = re[f], im[f], re[s], im[s]
        re[f] = (a0 * fr - a3 * fi) + (a2 * sr - a1 * si)
        im[f] = (a0 * fi + a3 * fr) + (a2 * si + a1 * sr)
        re[s] = (a0 * sr + a3 * si) - (a2 * fr + a1 * fi)
        im[s] = (a0 * si - a3 * sr) + (a1 * fr - a2 * fi)
    return re, im


def antihermitian_squares(moment):
    re, im = moment
    total = None
    for a, b in PAIRS:
        dr = re[3 * a + b] - re[3 * b + a]
        di = im[3 * a + b] + im[3 * b + a]
        term = dr * dr + di * di
        total = term if total is None else total + term
    third = (im[0] + im[4] + im[8]) * (1.0 / 3.0)
    total = 0.5 * total
    for a in range(3):
        part = im[4 * a] - third
        total = total + part * part
    return total


def sweep_kernel(pairs, own_tiles, width, *refs):
    own = refs[0:pairs]
    below = refs[pairs : 2 * pairs]
    above = refs[2 * pairs : 3 * pairs]
    gauge_out, sums_out = refs[3 * pairs : 3 * pairs + 2]
    flat, extra, link, staple_link, field, moved, scores = refs[3 * pairs + 2 :]
    rows = pairs * WINDOW
    per_pair = WINDOW * TILES
    stride = pairs * per_pair
    start = width
    first_own = start // LANES
    masks = Masks(rows)

    for part in range(PARTS):
        for colour in range(2):
            for p in range(pairs):
                base = (colour * PARTS + part) * stride + p * per_pair
                flat[pl.ds(base + 1, TILES), :] = below[p][
                    pl.ds(part * TILES * 2 + colour, TILES, stride=2), :
                ]
                flat[pl.ds(base + first_own, own_tiles), :] = own[p][
                    pl.ds(part * own_tiles * 2 + colour, own_tiles, stride=2), :
                ]
                flat[pl.ds(base + per_pair - TILES, TILES), :] = above[p][
                    pl.ds(part * TILES * 2 + colour, TILES, stride=2), :
                ]
    for p in range(pairs):
        for i in range(2 * COORDS):
            extra[pl.ds(i * rows + WINDOW * p, 1), :] = below[p][pl.ds(PARTS * TILES * 2 + i, 1), :]
        for i in range(COORDS):
            ahead = WINDOW * ((p + 1) % pairs)
            extra[pl.ds((2 * COORDS + i) * rows + ahead, 1), :] = above[p][
                pl.ds(PARTS * TILES * 2 + i, 1), :
            ]

    first_block = masks.block == 0
    low_lanes = masks.lane < HALF
    low_second = (masks.block == 1) & low_lanes
    low_first = first_block & low_lanes

    def loaded(colour, part, j):
        base = (colour * PARTS + part) * stride
        value = flat[pl.ds(base + j, rows, stride=TILES), :]
        edge_y = ROW_Y <= part < ROW_Y + COORDS
        edge_g = part >= GAUGE_AT
        if j == 0:
            fill = jnp.zeros_like(value)
            if colour == 1 and edge_g:
                fill = extra[pl.ds((2 * COORDS + part - GAUGE_AT) * rows, rows), :]
            value = jnp.where(first_block, fill, value)
        if j == 1:
            value = jnp.where(low_second, row_roll(value, 1), value)
            if colour == 1 and (edge_y or edge_g):
                at = part - ROW_Y if edge_y else COORDS + part - GAUGE_AT
                value = jnp.where(low_first, extra[pl.ds(at * rows, rows), :], value)
        return value

    for colour in range(2):
        for matrix in range(4):
            target = link if matrix < 3 else field
            at = (colour * 3 + matrix) * 18 if matrix < 3 else colour * 18
            for j in range(TILES):
                coords = [loaded(colour, matrix * COORDS + i, j) for i in range(COORDS)]
                re, im = decode(coords)
                for i in range(9):
                    target[at + i, :, tile_of(j)] = re[i]
                    target[at + 9 + i, :, tile_of(j)] = im[i]

    def read(ref, at):
        return [ref[at, :, tile_of(j)] for j in range(TILES)]

    def write(ref, at, tiles):
        for j in range(TILES):
            ref[at, :, tile_of(j)] = tiles[j]

    def keep(colour, direction, entry, re, im):
        at = (colour * 6 + direction) * 27 + entry
        write(staple_link, at, re)
        write(staple_link, at + 9, [im[j] - re[j] for j in range(TILES)])
        write(staple_link, at + 18, [im[j] + re[j] for j in range(TILES)])

    for colour in range(2):
        for a in range(3):
            for c in range(3):
                here = 3 * a + c
                there = 3 * c + a
                same = []
                other = []
                for reim in range(2):
                    ours = read(link, colour * 3 * 18 + reim * 9 + here)
                    theirs = read(link, (1 - colour) * 3 * 18 + reim * 9 + there)
                    if reim:
                        theirs = [-t for t in theirs]
                    behind = [row_roll(t, WINDOW) for t in theirs]
                    lower = [masks.odd(j) if colour else ~masks.odd(j) for j in range(TILES)]
                    same.append([jnp.where(lower[j], ours[j], theirs[j]) for j in range(TILES)])
                    other.append([jnp.where(lower[j], behind[j], ours[j]) for j in range(TILES)])
                keep(colour, 0, here, *same)
                keep(colour, 1, here, *other)
                for axis, shift in ((1, y_behind), (2, z_behind)):
                    at = (colour * 3 + axis) * 18 + here
                    keep(colour, 2 * axis, here, read(link, at), read(link, at + 9))
                    at = ((1 - colour) * 3 + axis) * 18 + there
                    re = shift(read(link, at), masks)
                    im = [-t for t in shift(read(link, at + 9), masks)]
                    keep(colour, 2 * axis + 1, here, re, im)

    def move(colour):
        for i in range(18):
            tiles = read(field, colour * 18 + i)
            behind = [row_roll(t, WINDOW) for t in tiles]
            if 2 * WINDOW == rows:
                other = behind
            else:
                other = []
                for j in range(TILES):
                    lower = ~masks.odd(j) if colour else masks.odd(j)
                    other.append(jnp.where(lower, behind[j], row_roll(tiles[j], -WINDOW)))
            at = colour * 5 * 18 + i
            write(moved, at, other)
            write(moved, at + 18, y_ahead(tiles, masks))
            write(moved, at + 36, y_behind(tiles, masks))
            write(moved, at + 54, z_ahead(tiles, masks))
            write(moved, at + 72, z_behind(tiles, masks))

    def matrix_at(ref, at, group, j):
        block = [ref[at + i, group, tile_of(j)] for i in range(18)]
        return block[:9], block[9:]

    def moment_of(colour, group, j):
        them = 1 - colour
        sums = None
        for direction in range(6):
            if direction == 0:
                right = matrix_at(field, them * 18, group, j)
            else:
                right = matrix_at(moved, (them * 5 + direction - 1) * 18, group, j)
            at = (colour * 6 + direction) * 27
            entries = [staple_link[at + i, group, tile_of(j)] for i in range(27)]
            sums = add_staple(sums, (entries[:9], entries[9:18], entries[18:]), right)
        total = (
            [sums[0][i] + sums[1][i] for i in range(9)],
            [sums[2][i] - sums[0][i] for i in range(9)],
        )
        gauge = matrix_at(field, colour * 18, group, j)
        return gauge, times(gauge, total)

    def groups(body, init):
        count = rows // 8
        if count == 1:
            return body(0, pl.ds(0, 8), init)
        return lax.fori_loop(
            0, count, lambda g, carry: body(g, pl.ds(pl.multiple_of(g * 8, 8), 8), carry), init
        )

    group_masks = Masks(8)
    owned = [group_masks.owned(j, start, width) for j in range(TILES)]
    zero = jnp.zeros((8, LANES), jnp.float32)

    def half_sweep(colour, last=False):
        def body(g, group, carry):
            score, squares = carry
            for j in range(TILES):
                gauge, moment = moment_of(colour, group, j)
                for one, two in PAIRS:
                    coeffs = relax_coeffs(moment, one, two)
                    gauge = turn_rows(gauge, one, two, coeffs)
                    moment = turn_rows(moment, one, two, coeffs)
                for i in range(9):
                    field[colour * 18 + i, group, tile_of(j)] = gauge[0][i]
                    field[colour * 18 + 9 + i, group, tile_of(j)] = gauge[1][i]
                if colour == 1:
                    trace = moment[0][0] + moment[0][4] + moment[0][8]
                    score = score + jnp.where(owned[j], trace, 0.0)
                if last:
                    squares = squares + jnp.where(owned[j], antihermitian_squares(moment), 0.0)
            return score, squares

        return groups(body, (zero, zero))

    move(1)

    def iteration(k, carry):
        half_sweep(0)
        move(0)
        scores[k], _ = half_sweep(1)
        move(1)
        return carry

    lax.fori_loop(0, ITERS - 1, iteration, 0)
    half_sweep(0)
    move(0)
    scores[ITERS - 1], scores[ITERS] = half_sweep(1, last=True)
    move(1)

    def theta_body(g, group, squares):
        for j in range(TILES):
            _, moment = moment_of(0, group, j)
            squares = squares + jnp.where(owned[j], antihermitian_squares(moment), 0.0)
        return squares

    scores[ITERS] = groups(theta_body, scores[ITERS])

    line = lax.broadcasted_iota(jnp.int32, (8, LANES), 0)
    column = lax.broadcasted_iota(jnp.int32, (8, LANES), 1)
    sums = jnp.where(line == 1, jnp.sum(scores[ITERS]), 0.0)
    for k in range(ITERS):
        sums = jnp.where((line == 0) & (column == k), jnp.sum(scores[k]), sums)
    sums_out[...] = sums

    tile_line = lax.broadcasted_iota(jnp.int32, (own_tiles, LANES), 0)
    tile_lane = lax.broadcasted_iota(jnp.int32, (own_tiles, LANES), 1)
    place = tile_line * LANES + tile_lane
    odd = (place // NZ + place % NZ) % 2 == 1
    low = tile_lane < HALF
    for i in range(18):
        colours = []
        for colour in range(2):
            base = (colour * PARTS + i) * stride
            for j in range(TILES):
                flat[pl.ds(base + j, rows, stride=TILES), :] = field[colour * 18 + i, :, tile_of(j)]
            early = flat[pl.ds(base + first_own, own_tiles), :]
            late = flat[pl.ds(base + first_own + 1, own_tiles), :]
            colours.append(jnp.where(low, lane_roll(early, HALF), lane_roll(late, HALF)))
        planes = (
            jnp.where(odd, colours[1], colours[0]),
            jnp.where(odd, colours[0], colours[1]),
        )
        for x in range(2):
            for t in range(own_tiles):
                size = min(LANES, width - t * LANES)
                gauge_out[i, x : x + 1, t * LANES : t * LANES + size] = planes[x][
                    t : t + 1, :size
                ]


def sweeps(own, below, above, width):
    pairs = len(own)
    own_tiles = -(-width // LANES)
    rows = pairs * WINDOW
    stride = pairs * WINDOW * TILES
    cells = lambda count: pltpu.VMEM((count, rows, BLOCK), jnp.float32)
    return pl.pallas_call(
        lambda *refs: sweep_kernel(pairs, own_tiles, width, *refs),
        out_shape=[
            jax.ShapeDtypeStruct((18, 2, width), jnp.float32),
            jax.ShapeDtypeStruct((8, LANES), jnp.float32),
        ],
        scratch_shapes=[
            pltpu.VMEM((2 * PARTS * stride, LANES), jnp.float32),
            pltpu.VMEM((3 * COORDS * rows, LANES), jnp.float32),
            cells(2 * 3 * 18),
            cells(2 * 6 * 27),
            cells(2 * 18),
            cells(2 * 5 * 18),
            pltpu.VMEM((8, 8, LANES), jnp.float32),
        ],
        compiler_params=pltpu.CompilerParams(vmem_limit_bytes=(pairs * 7 + 2) << 20),
        name="sweeps",
    )(*own, *below, *above)


def rotate_kernel(here, links, ahead, gauge, out):
    def matrix(ref):
        return [ref[i] for i in range(9)], [ref[9 + i] for i in range(9)]

    gauge[...] = here[...]
    re, im = times_dagger(times(matrix(here), matrix(links)), matrix(ahead))
    for i in range(9):
        out[i] = re[i]
        out[9 + i] = im[i]


def rotate(here, links, ahead):
    shape = jax.ShapeDtypeStruct(here.shape, here.dtype)
    return pl.pallas_call(
        rotate_kernel,
        out_shape=[shape, shape],
        compiler_params=pltpu.CompilerParams(vmem_limit_bytes=6 << 20),
        name="rotate",
    )(here, links, ahead)


def finish_kernel(volume, ours, theirs, functional, theta):
    total = ours[...] + theirs[...]
    functional[...] = total[:1, :ITERS] * (1.0 / (9.0 * volume))
    theta[...] = total[1:2, :1] * (1.0 / (3.0 * volume))


def finish(ours, theirs, volume):
    return pl.pallas_call(
        lambda *refs: finish_kernel(volume, *refs),
        out_shape=[
            jax.ShapeDtypeStruct((1, ITERS), jnp.float32),
            jax.ShapeDtypeStruct((1, 1), jnp.float32),
        ],
        compiler_params=pltpu.CompilerParams(vmem_limit_bytes=1 << 20),
        name="finish",
    )(ours, theirs)


def from_ahead(block, axis, distance):
    count = lax.axis_size(axis)
    return lax.ppermute(block, axis, [((i + distance) % count, i) for i in range(count)])


def fixed(space_links, time_links, start_gauge):
    x_sites, width = start_gauge.shape[-2:]
    pairs = lax.axis_size("gx")
    volume = x_sites * pairs * width * lax.axis_size("gy")
    assert x_sites == 2 and start_gauge.shape[3] == 1
    assert width % NZ == 0 and (width // NZ) % 2 == 0 and width % LANES == HALF
    assert 2 * width + BLOCK == WINDOW * BLOCK and pairs >= 2
    assert BLOCK_ROWS >= 2 * ITERS

    own, below, above = pack(
        space_links.reshape(54, x_sites, width), start_gauge.reshape(18, x_sites, width)
    )
    below = from_ahead(below, "gy", -1)
    above = from_ahead(above, "gy", 1)
    owns, belows, aboves = [own], [below], [above]
    for i in range(1, pairs):
        owns.append(from_ahead(own, "gx", i))
        belows.append(from_ahead(below, "gx", i))
        aboves.append(from_ahead(above, "gx", i))
    gauge, sums = sweeps(owns, belows, aboves, width)
    ahead = from_ahead(gauge, "ta", 1)
    count = lax.axis_size("gy")
    theirs = jnp.zeros_like(sums)
    if count & (count - 1) == 0:
        step = 1
        while step < count:
            theirs = lax.ppermute(sums, "gy", [(i, i ^ step) for i in range(count)])
            step *= 2
            if step < count:
                sums = sums + theirs
    else:
        theirs = sum(from_ahead(sums, "gy", i) for i in range(1, count))
    gauge, rotated = rotate(gauge, time_links.reshape(18, x_sites, width), ahead)
    functional, theta = finish(sums, theirs, volume)
    shape = start_gauge.shape
    return gauge.reshape(shape), rotated.reshape(shape), functional.reshape(ITERS, 1), theta.reshape(1)


def solution(mesh):
    placed = (
        P(None, None, None, None, "ta", "gx", "gy"),
        P(None, None, None, "ta", "gx", "gy"),
        P(None, None, None, "ta", "gx", "gy"),
    )
    return jax.shard_map(
        fixed,
        mesh=mesh,
        in_specs=placed,
        out_specs=(
            P(None, None, None, "ta", "gx", "gy"),
            P(None, None, None, "ta", "gx", "gy"),
            P(None, "ta"),
            P("ta"),
        ),
        check_vma=False,
    )
```

```python
import math

import jax
import jax.numpy as jnp
from jax import lax
from jax.experimental import pallas as pl
from jax.experimental.pallas import tpu as pltpu
from jax.sharding import PartitionSpec as P


NZ = 48
ITERS = 4

OMEGA = 1.7
FLOOR = 0.5
PAIRS = ((0, 1), (1, 2), (0, 2))

LANES = 128
HALF = LANES // 2
BLOCK_ROWS = LANES // math.gcd(NZ, LANES)
TILES = BLOCK_ROWS * NZ // LANES
BLOCK = BLOCK_ROWS * NZ
WINDOW = 4
COORDS = 8
PARTS = 4 * COORDS
ROW_Y = COORDS
GAUGE_AT = 3 * COORDS
POLE = 1e15
NEAR_POLE = 1e-30


def to_plane(point):
    first, rest = point[0], point[1:]
    square = rest[0] * rest[0]
    for entry in rest[1:]:
        square = square + entry * entry
    upper = first >= 0.0
    top = jnp.where(upper, 1.0, 1.0 - first)
    bottom = jnp.where(upper, 1.0 + first, jnp.maximum(square, NEAR_POLE))
    scale = top / bottom
    plane = [scale * entry for entry in rest]
    at_pole = (first < 0.0) & (square < NEAR_POLE)
    plane[0] = jnp.where(at_pole, POLE, plane[0])
    return plane


def from_plane(plane):
    square = plane[0] * plane[0]
    for entry in plane[1:]:
        square = square + entry * entry
    scale = 2.0 / (1.0 + square)
    return scale, [scale - 1.0] + [scale * entry for entry in plane]


def row_and_basis(plane):
    scale, point = from_plane(plane)
    row = [(point[0], point[1]), (point[2], point[3]), (point[4], point[5])]
    u = [(scale, point[1]), row[1], row[2]]
    tilt = plane[0]
    inverse = 1.0 / (1.0 + tilt * tilt)
    basis = []
    for j in (1, 2):
        re, im = plane[2 * j - 1], plane[2 * j]
        zr = (re + im * tilt) * inverse
        zi = (re * tilt - im) * inverse
        vector = []
        for k in range(3):
            ur, ui = u[k]
            br = ui * zi - ur * zr
            bi = -(ur * zi + ui * zr)
            vector.append((1.0 + br, bi) if k == j else (br, bi))
        basis.append(vector)
    return row, basis


def encode(first, second):
    point = [part for entry in first for part in entry]
    plane = to_plane(point)
    _, basis = row_and_basis(plane)
    coeffs = []
    for vector in basis:
        re = im = None
        for (sr, si), (br, bi) in zip(second, vector):
            tr = sr * br + si * bi
            ti = si * br - sr * bi
            re = tr if re is None else re + tr
            im = ti if im is None else im + ti
        coeffs += [re, im]
    return plane + to_plane(coeffs)


def decode(coords):
    first, basis = row_and_basis(coords[:5])
    _, coeffs = from_plane(coords[5:])
    second = []
    for k in range(3):
        re = im = None
        for j in range(2):
            cr, ci = coeffs[2 * j], coeffs[2 * j + 1]
            br, bi = basis[j][k]
            tr = cr * br - ci * bi
            ti = cr * bi + ci * br
            re = tr if re is None else re + tr
            im = ti if im is None else im + ti
        second.append((re, im))
    third = []
    for i in range(3):
        (ar, ai), (cr, ci) = first[(i + 1) % 3], first[(i + 2) % 3]
        (br, bi), (dr, di) = second[(i + 1) % 3], second[(i + 2) % 3]
        re = (ar * dr - ai * di) - (cr * br - ci * bi)
        im = (cr * bi + ci * br) - (ar * di + ai * dr)
        third.append((re, im))
    rows = first + second + third
    return [entry[0] for entry in rows], [entry[1] for entry in rows]


def pack_kernel(
    own_tiles, links_hbm, gauge_hbm, own, below, above, links, gauge, natural, coded, arrived
):
    copies = [
        pltpu.make_async_copy(
            links_hbm.at[pl.ds(18 * axis, 18)], links.at[pl.ds(18 * axis, 18)], arrived.at[axis]
        )
        for axis in range(3)
    ]
    copies.append(pltpu.make_async_copy(gauge_hbm, gauge, arrived.at[3]))
    for copy in copies:
        copy.start()
    width = gauge.shape[-1]
    last = width - (own_tiles - 1) * LANES
    lane = lax.broadcasted_iota(jnp.int32, (2, width), 1)
    odd = (lane // NZ + lane % NZ) % 2 == 1
    rows = 2 * own_tiles
    for matrix in range(4):
        copies[matrix].wait()
        for number in range(12):
            entry = number if number < 6 else number + 3
            both = gauge[entry] if matrix == 3 else links[matrix * 18 + entry]
            swapped = jnp.concatenate([both[1:2], both[0:1]], axis=0)
            packed = jnp.where(odd, swapped, both)
            for t in range(own_tiles):
                tile = packed[:, t * LANES : (t + 1) * LANES]
                if t == own_tiles - 1:
                    tile = jnp.concatenate([tile, jnp.zeros((2, LANES - last), jnp.float32)], axis=1)
                natural[pl.ds((matrix * 12 + number) * rows + 2 * t, 2), :] = tile
        values = [natural[pl.ds((matrix * 12 + i) * rows, rows), :] for i in range(12)]
        entries = [(values[i], values[6 + i]) for i in range(6)]
        for i, value in enumerate(encode(entries[:3], entries[3:])):
            coded[pl.ds(8 + (matrix * COORDS + i) * rows, rows), :] = value
    low = lax.broadcasted_iota(jnp.int32, (rows, LANES), 1) < HALF
    first = own_tiles - 1 - TILES
    extra_below = extra_above = PARTS * TILES * 2
    for part in range(PARTS):
        base = 8 + part * rows
        here = pltpu.roll(coded[pl.ds(base, rows), :], HALF, 1)
        before = pltpu.roll(coded[pl.ds(base - 2, rows), :], HALF, 1)
        own[pl.ds(part * rows, rows), :] = jnp.where(low, before, here)
        at = part * TILES * 2
        edge = jnp.where(
            low[:2],
            coded[pl.ds(base + 2 * (own_tiles - 1), 2), :],
            coded[pl.ds(base + 2 * first, 2), :],
        )
        below[pl.ds(at, 2), :] = edge
        below[pl.ds(at + 2, 2 * TILES - 2), :] = coded[
            pl.ds(base + 2 * first + 2, 2 * TILES - 2), :
        ]
        above[pl.ds(at, 2 * TILES), :] = coded[pl.ds(base, 2 * TILES), :]
        if ROW_Y <= part < ROW_Y + COORDS or part >= GAUGE_AT:
            below[pl.ds(extra_below, 1), :] = coded[pl.ds(base + 2 * first + 1, 1), :]
            extra_below += 1
        if part >= GAUGE_AT:
            above[pl.ds(extra_above, 1), :] = coded[pl.ds(base + 2 * TILES + 1, 1), :]
            extra_above += 1


def pack(links, gauge):
    width = gauge.shape[-1]
    own_tiles = -(-width // LANES)
    rows = PARTS * TILES * 2
    shapes = [
        jax.ShapeDtypeStruct((PARTS * own_tiles * 2, LANES), jnp.float32),
        jax.ShapeDtypeStruct((rows + 2 * COORDS, LANES), jnp.float32),
        jax.ShapeDtypeStruct((rows + COORDS, LANES), jnp.float32),
    ]
    return pl.pallas_call(
        lambda *refs: pack_kernel(own_tiles, *refs),
        out_shape=shapes,
        in_specs=[pl.BlockSpec(memory_space=pltpu.HBM)] * 2,
        scratch_shapes=[
            pltpu.VMEM(links.shape, links.dtype),
            pltpu.VMEM(gauge.shape, gauge.dtype),
            pltpu.VMEM((48 * own_tiles * 2, LANES), jnp.float32),
            pltpu.VMEM((8 + PARTS * own_tiles * 2, LANES), jnp.float32),
            pltpu.SemaphoreType.DMA((4,)),
        ],
        compiler_params=pltpu.CompilerParams(vmem_limit_bytes=6 << 20),
        name="pack",
    )(*[pltpu.with_memory_space_constraint(value, pltpu.HBM) for value in (links, gauge)])


def row_roll(value, shift):
    return pltpu.roll(value, shift % value.shape[0], 0)


def lane_roll(value, shift):
    return pltpu.roll(value, shift % LANES, 1)


class Masks:
    def __init__(self, rows):
        self.lane = lax.broadcasted_iota(jnp.int32, (rows, LANES), 1)
        self.block = lax.broadcasted_iota(jnp.int32, (rows, LANES), 0) % WINDOW

    def z(self, tile):
        return (self.lane + tile * LANES) % NZ

    def odd(self, tile):
        return ((self.lane + tile * LANES) // NZ + self.z(tile)) % 2 == 1

    def owned(self, tile, start, width):
        place = self.block * BLOCK + tile * LANES + self.lane
        return (place >= start) & (place < start + width)


def y_ahead(tiles, masks):
    turned = [lane_roll(tile, -NZ) for tile in tiles]
    turned.append(row_roll(turned[0], -1))
    inside = masks.lane < LANES - NZ
    return [jnp.where(inside, turned[j], turned[j + 1]) for j in range(TILES)]


def y_behind(tiles, masks):
    turned = [lane_roll(tile, NZ) for tile in tiles]
    before = row_roll(turned[TILES - 1], 1)
    inside = masks.lane >= NZ
    return [jnp.where(inside, turned[j], turned[j - 1] if j else before) for j in range(TILES)]


def z_ahead(tiles, masks):
    step = [lane_roll(tile, -1) for tile in tiles]
    wrap = [lane_roll(tile, NZ - 1) for tile in tiles]
    out = []
    for j in range(TILES):
        near = step[j]
        if j < TILES - 1:
            near = jnp.where(masks.lane < LANES - 1, step[j], step[j + 1])
        far = wrap[j]
        if j:
            far = jnp.where(masks.lane >= NZ - 1, wrap[j], wrap[j - 1])
        out.append(jnp.where(masks.z(j) == NZ - 1, far, near))
    return out


def z_behind(tiles, masks):
    step = [lane_roll(tile, 1) for tile in tiles]
    wrap = [lane_roll(tile, 1 - NZ) for tile in tiles]
    out = []
    for j in range(TILES):
        near = step[j]
        if j:
            near = jnp.where(masks.lane >= 1, step[j], step[j - 1])
        far = wrap[j]
        if j < TILES - 1:
            far = jnp.where(masks.lane < LANES - NZ + 1, wrap[j], wrap[j + 1])
        out.append(jnp.where(masks.z(j) == 0, far, near))
    return out


def tile_of(j):
    return slice(j * LANES, (j + 1) * LANES)


def times_dagger(left, right):
    left_re, left_im = left
    right_re, right_im = right
    out_re = []
    out_im = []
    for a in range(3):
        for b in range(3):
            re = im = None
            for c in range(3):
                lr, li = left_re[3 * a + c], left_im[3 * a + c]
                rr, ri = right_re[3 * b + c], right_im[3 * b + c]
                re = lr * rr if re is None else re + lr * rr
                re = re + li * ri
                im = li * rr if im is None else im + li * rr
                im = im - lr * ri
            out_re.append(re)
            out_im.append(im)
    return out_re, out_im


def add_staple(sums, link, gauge):
    gauge_re, gauge_im = gauge
    both = [gauge_re[i] + gauge_im[i] for i in range(9)]
    right = (both, gauge_im, gauge_re)
    out = []
    for k in range(3):
        entries = []
        for a in range(3):
            for b in range(3):
                value = None if sums is None else sums[k][3 * a + b]
                for c in range(3):
                    term = link[k][3 * a + c] * right[k][3 * b + c]
                    value = term if value is None else value + term
                entries.append(value)
        out.append(entries)
    return out


def times(left, right):
    left_re, left_im = left
    right_re, right_im = right
    out_re = []
    out_im = []
    for a in range(3):
        for b in range(3):
            re = im = None
            for c in range(3):
                lr, li = left_re[3 * a + c], left_im[3 * a + c]
                rr, ri = right_re[3 * c + b], right_im[3 * c + b]
                re = lr * rr if re is None else re + lr * rr
                re = re - li * ri
                im = lr * ri if im is None else im + lr * ri
                im = im + li * rr
            out_re.append(re)
            out_im.append(im)
    return out_re, out_im


def relax_coeffs(moment, one, two):
    re, im = moment
    c0 = re[4 * one] + re[4 * two]
    c1 = -(im[3 * one + two] + im[3 * two + one])
    c2 = re[3 * two + one] - re[3 * one + two]
    c3 = im[4 * two] - im[4 * one]
    length = jnp.sqrt(c0 * c0 + c1 * c1 + c2 * c2 + c3 * c3)
    v0 = (1.0 - OMEGA) * length + OMEGA * c0
    v1 = OMEGA * c1
    v2 = OMEGA * c2
    v3 = OMEGA * c3
    scale = lax.rsqrt(jnp.maximum(v0 * v0 + v1 * v1 + v2 * v2 + v3 * v3, FLOOR * FLOOR))
    return v0 * scale, v1 * scale, v2 * scale, v3 * scale


def turn_rows(matrix, one, two, coeffs):
    a0, a1, a2, a3 = coeffs
    re = list(matrix[0])
    im = list(matrix[1])
    for col in range(3):
        f, s = 3 * one + col, 3 * two + col
        fr, fi, sr, si = re[f], im[f], re[s], im[s]
        re[f] = (a0 * fr - a3 * fi) + (a2 * sr - a1 * si)
        im[f] = (a0 * fi + a3 * fr) + (a2 * si + a1 * sr)
        re[s] = (a0 * sr + a3 * si) - (a2 * fr + a1 * fi)
        im[s] = (a0 * si - a3 * sr) + (a1 * fr - a2 * fi)
    return re, im


def antihermitian_squares(moment):
    re, im = moment
    total = None
    for a, b in PAIRS:
        dr = re[3 * a + b] - re[3 * b + a]
        di = im[3 * a + b] + im[3 * b + a]
        term = dr * dr + di * di
        total = term if total is None else total + term
    third = (im[0] + im[4] + im[8]) * (1.0 / 3.0)
    total = 0.5 * total
    for a in range(3):
        part = im[4 * a] - third
        total = total + part * part
    return total


def sweep_kernel(pairs, own_tiles, width, *refs):
    own = refs[0:pairs]
    below = refs[pairs : 2 * pairs]
    above = refs[2 * pairs : 3 * pairs]
    gauge_out, sums_out = refs[3 * pairs : 3 * pairs + 2]
    flat, extra, link, staple_link, field, moved, scores = refs[3 * pairs + 2 :]
    rows = pairs * WINDOW
    per_pair = WINDOW * TILES
    stride = pairs * per_pair
    start = width
    first_own = start // LANES
    masks = Masks(rows)

    for part in range(PARTS):
        for colour in range(2):
            for p in range(pairs):
                base = (colour * PARTS + part) * stride + p * per_pair
                flat[pl.ds(base + 1, TILES), :] = below[p][
                    pl.ds(part * TILES * 2 + colour, TILES, stride=2), :
                ]
                flat[pl.ds(base + first_own, own_tiles), :] = own[p][
                    pl.ds(part * own_tiles * 2 + colour, own_tiles, stride=2), :
                ]
                flat[pl.ds(base + per_pair - TILES, TILES), :] = above[p][
                    pl.ds(part * TILES * 2 + colour, TILES, stride=2), :
                ]
    for p in range(pairs):
        for i in range(2 * COORDS):
            extra[pl.ds(i * rows + WINDOW * p, 1), :] = below[p][pl.ds(PARTS * TILES * 2 + i, 1), :]
        for i in range(COORDS):
            ahead = WINDOW * ((p + 1) % pairs)
            extra[pl.ds((2 * COORDS + i) * rows + ahead, 1), :] = above[p][
                pl.ds(PARTS * TILES * 2 + i, 1), :
            ]

    first_block = masks.block == 0
    low_lanes = masks.lane < HALF
    low_second = (masks.block == 1) & low_lanes
    low_first = first_block & low_lanes

    def loaded(colour, part, j):
        base = (colour * PARTS + part) * stride
        value = flat[pl.ds(base + j, rows, stride=TILES), :]
        edge_y = ROW_Y <= part < ROW_Y + COORDS
        edge_g = part >= GAUGE_AT
        if j == 0:
            fill = jnp.zeros_like(value)
            if colour == 1 and edge_g:
                fill = extra[pl.ds((2 * COORDS + part - GAUGE_AT) * rows, rows), :]
            value = jnp.where(first_block, fill, value)
        if j == 1:
            value = jnp.where(low_second, row_roll(value, 1), value)
            if colour == 1 and (edge_y or edge_g):
                at = part - ROW_Y if edge_y else COORDS + part - GAUGE_AT
                value = jnp.where(low_first, extra[pl.ds(at * rows, rows), :], value)
        return value

    for colour in range(2):
        for matrix in range(4):
            target = link if matrix < 3 else field
            at = (colour * 3 + matrix) * 18 if matrix < 3 else colour * 18
            for j in range(TILES):
                coords = [loaded(colour, matrix * COORDS + i, j) for i in range(COORDS)]
                re, im = decode(coords)
                for i in range(9):
                    target[at + i, :, tile_of(j)] = re[i]
                    target[at + 9 + i, :, tile_of(j)] = im[i]

    def read(ref, at):
        return [ref[at, :, tile_of(j)] for j in range(TILES)]

    def write(ref, at, tiles):
        for j in range(TILES):
            ref[at, :, tile_of(j)] = tiles[j]

    def keep(colour, direction, entry, re, im):
        at = (colour * 6 + direction) * 27 + entry
        write(staple_link, at, re)
        write(staple_link, at + 9, [im[j] - re[j] for j in range(TILES)])
        write(staple_link, at + 18, [im[j] + re[j] for j in range(TILES)])

    for colour in range(2):
        for a in range(3):
            for c in range(3):
                here = 3 * a + c
                there = 3 * c + a
                same = []
                other = []
                for reim in range(2):
                    ours = read(link, colour * 3 * 18 + reim * 9 + here)
                    theirs = read(link, (1 - colour) * 3 * 18 + reim * 9 + there)
                    if reim:
                        theirs = [-t for t in theirs]
                    behind = [row_roll(t, WINDOW) for t in theirs]
                    lower = [masks.odd(j) if colour else ~masks.odd(j) for j in range(TILES)]
                    same.append([jnp.where(lower[j], ours[j], theirs[j]) for j in range(TILES)])
                    other.append([jnp.where(lower[j], behind[j], ours[j]) for j in range(TILES)])
                keep(colour, 0, here, *same)
                keep(colour, 1, here, *other)
                for axis, shift in ((1, y_behind), (2, z_behind)):
                    at = (colour * 3 + axis) * 18 + here
                    keep(colour, 2 * axis, here, read(link, at), read(link, at + 9))
                    at = ((1 - colour) * 3 + axis) * 18 + there
                    re = shift(read(link, at), masks)
                    im = [-t for t in shift(read(link, at + 9), masks)]
                    keep(colour, 2 * axis + 1, here, re, im)

    def move(colour):
        for i in range(18):
            tiles = read(field, colour * 18 + i)
            behind = [row_roll(t, WINDOW) for t in tiles]
            if 2 * WINDOW == rows:
                other = behind
            else:
                other = []
                for j in range(TILES):
                    lower = ~masks.odd(j) if colour else masks.odd(j)
                    other.append(jnp.where(lower, behind[j], row_roll(tiles[j], -WINDOW)))
            at = colour * 5 * 18 + i
            write(moved, at, other)
            write(moved, at + 18, y_ahead(tiles, masks))
            write(moved, at + 36, y_behind(tiles, masks))
            write(moved, at + 54, z_ahead(tiles, masks))
            write(moved, at + 72, z_behind(tiles, masks))

    def matrix_at(ref, at, group, j):
        block = [ref[at + i, group, tile_of(j)] for i in range(18)]
        return block[:9], block[9:]

    def moment_of(colour, group, j):
        them = 1 - colour
        sums = None
        for direction in range(6):
            if direction == 0:
                right = matrix_at(field, them * 18, group, j)
            else:
                right = matrix_at(moved, (them * 5 + direction - 1) * 18, group, j)
            at = (colour * 6 + direction) * 27
            entries = [staple_link[at + i, group, tile_of(j)] for i in range(27)]
            sums = add_staple(sums, (entries[:9], entries[9:18], entries[18:]), right)
        total = (
            [sums[0][i] + sums[1][i] for i in range(9)],
            [sums[2][i] - sums[0][i] for i in range(9)],
        )
        gauge = matrix_at(field, colour * 18, group, j)
        return gauge, times(gauge, total)

    def groups(body, init):
        count = rows // 8
        if count == 1:
            return body(0, pl.ds(0, 8), init)
        return lax.fori_loop(
            0, count, lambda g, carry: body(g, pl.ds(pl.multiple_of(g * 8, 8), 8), carry), init
        )

    group_masks = Masks(8)
    owned = [group_masks.owned(j, start, width) for j in range(TILES)]
    zero = jnp.zeros((8, LANES), jnp.float32)

    def half_sweep(colour, last=False):
        def body(g, group, carry):
            score, squares = carry
            for j in range(TILES):
                gauge, moment = moment_of(colour, group, j)
                for one, two in PAIRS:
                    coeffs = relax_coeffs(moment, one, two)
                    gauge = turn_rows(gauge, one, two, coeffs)
                    moment = turn_rows(moment, one, two, coeffs)
                for i in range(9):
                    field[colour * 18 + i, group, tile_of(j)] = gauge[0][i]
                    field[colour * 18 + 9 + i, group, tile_of(j)] = gauge[1][i]
                if colour == 1:
                    trace = moment[0][0] + moment[0][4] + moment[0][8]
                    score = score + jnp.where(owned[j], trace, 0.0)
                if last:
                    squares = squares + jnp.where(owned[j], antihermitian_squares(moment), 0.0)
            return score, squares

        return groups(body, (zero, zero))

    move(1)

    for k in range(ITERS):
        half_sweep(0)
        move(0)
        scores[k], scores[ITERS] = half_sweep(1, last=k == ITERS - 1)
        move(1)

    tile_line = lax.broadcasted_iota(jnp.int32, (own_tiles, LANES), 0)
    tile_lane = lax.broadcasted_iota(jnp.int32, (own_tiles, LANES), 1)
    place = tile_line * LANES + tile_lane
    odd = (place // NZ + place % NZ) % 2 == 1
    low = tile_lane < HALF
    for i in range(18):
        colours = []
        for colour in range(2):
            base = (colour * PARTS + i) * stride
            for j in range(TILES):
                flat[pl.ds(base + j, rows, stride=TILES), :] = field[colour * 18 + i, :, tile_of(j)]
            early = flat[pl.ds(base + first_own, own_tiles), :]
            late = flat[pl.ds(base + first_own + 1, own_tiles), :]
            colours.append(jnp.where(low, lane_roll(early, HALF), lane_roll(late, HALF)))
        planes = (
            jnp.where(odd, colours[1], colours[0]),
            jnp.where(odd, colours[0], colours[1]),
        )
        for x in range(2):
            for t in range(own_tiles):
                size = min(LANES, width - t * LANES)
                gauge_out[i, x : x + 1, t * LANES : t * LANES + size] = planes[x][
                    t : t + 1, :size
                ]

    def theta_body(g, group, squares):
        for j in range(TILES):
            _, moment = moment_of(0, group, j)
            squares = squares + jnp.where(owned[j], antihermitian_squares(moment), 0.0)
        return squares

    scores[ITERS] = groups(theta_body, scores[ITERS])

    line = lax.broadcasted_iota(jnp.int32, (8, LANES), 0)
    column = lax.broadcasted_iota(jnp.int32, (8, LANES), 1)
    sums = jnp.where(line == 1, jnp.sum(scores[ITERS]), 0.0)
    for k in range(ITERS):
        sums = jnp.where((line == 0) & (column == k), jnp.sum(scores[k]), sums)
    sums_out[...] = sums


def sweeps(own, below, above, width):
    pairs = len(own)
    own_tiles = -(-width // LANES)
    rows = pairs * WINDOW
    stride = pairs * WINDOW * TILES
    cells = lambda count: pltpu.VMEM((count, rows, BLOCK), jnp.float32)
    return pl.pallas_call(
        lambda *refs: sweep_kernel(pairs, own_tiles, width, *refs),
        out_shape=[
            jax.ShapeDtypeStruct((18, 2, width), jnp.float32),
            jax.ShapeDtypeStruct((8, LANES), jnp.float32),
        ],
        scratch_shapes=[
            pltpu.VMEM((2 * PARTS * stride, LANES), jnp.float32),
            pltpu.VMEM((3 * COORDS * rows, LANES), jnp.float32),
            cells(2 * 3 * 18),
            cells(2 * 6 * 27),
            cells(2 * 18),
            cells(2 * 5 * 18),
            pltpu.VMEM((8, 8, LANES), jnp.float32),
        ],
        compiler_params=pltpu.CompilerParams(vmem_limit_bytes=(pairs * 7 + 2) << 20),
        name="sweeps",
    )(*own, *below, *above)


def rotate_kernel(here, links, ahead, gauge, out):
    def matrix(ref):
        return [ref[i] for i in range(9)], [ref[9 + i] for i in range(9)]

    gauge[...] = here[...]
    re, im = times_dagger(times(matrix(here), matrix(links)), matrix(ahead))
    for i in range(9):
        out[i] = re[i]
        out[9 + i] = im[i]


def rotate(here, links, ahead):
    shape = jax.ShapeDtypeStruct(here.shape, here.dtype)
    return pl.pallas_call(
        rotate_kernel,
        out_shape=[shape, shape],
        compiler_params=pltpu.CompilerParams(vmem_limit_bytes=6 << 20),
        name="rotate",
    )(here, links, ahead)


def finish_kernel(volume, ours, theirs, functional, theta):
    total = ours[...] + theirs[...]
    functional[...] = total[:1, :ITERS] * (1.0 / (9.0 * volume))
    theta[...] = total[1:2, :1] * (1.0 / (3.0 * volume))


def finish(ours, theirs, volume):
    return pl.pallas_call(
        lambda *refs: finish_kernel(volume, *refs),
        out_shape=[
            jax.ShapeDtypeStruct((1, ITERS), jnp.float32),
            jax.ShapeDtypeStruct((1, 1), jnp.float32),
        ],
        compiler_params=pltpu.CompilerParams(vmem_limit_bytes=1 << 20),
        name="finish",
    )(ours, theirs)


def from_ahead(block, axis, distance):
    count = lax.axis_size(axis)
    return lax.ppermute(block, axis, [((i + distance) % count, i) for i in range(count)])


def fixed(space_links, time_links, start_gauge):
    x_sites, width = start_gauge.shape[-2:]
    pairs = lax.axis_size("gx")
    volume = x_sites * pairs * width * lax.axis_size("gy")
    assert x_sites == 2 and start_gauge.shape[3] == 1
    assert width % NZ == 0 and (width // NZ) % 2 == 0 and width % LANES == HALF
    assert 2 * width + BLOCK == WINDOW * BLOCK and pairs >= 2
    assert BLOCK_ROWS >= 2 * ITERS

    own, below, above = pack(
        space_links.reshape(54, x_sites, width), start_gauge.reshape(18, x_sites, width)
    )
    below = from_ahead(below, "gy", -1)
    above = from_ahead(above, "gy", 1)
    owns, belows, aboves = [own], [below], [above]
    for i in range(1, pairs):
        owns.append(from_ahead(own, "gx", i))
        belows.append(from_ahead(below, "gx", i))
        aboves.append(from_ahead(above, "gx", i))
    gauge, sums = sweeps(owns, belows, aboves, width)
    ahead = from_ahead(gauge, "ta", 1)
    count = lax.axis_size("gy")
    theirs = jnp.zeros_like(sums)
    if count & (count - 1) == 0:
        step = 1
        while step < count:
            theirs = lax.ppermute(sums, "gy", [(i, i ^ step) for i in range(count)])
            step *= 2
            if step < count:
                sums = sums + theirs
    else:
        theirs = sum(from_ahead(sums, "gy", i) for i in range(1, count))
    gauge, rotated = rotate(gauge, time_links.reshape(18, x_sites, width), ahead)
    functional, theta = finish(sums, theirs, volume)
    shape = start_gauge.shape
    return gauge.reshape(shape), rotated.reshape(shape), functional.reshape(ITERS, 1), theta.reshape(1)


def solution(mesh):
    placed = (
        P(None, None, None, None, "ta", "gx", "gy"),
        P(None, None, None, "ta", "gx", "gy"),
        P(None, None, None, "ta", "gx", "gy"),
    )
    return jax.shard_map(
        fixed,
        mesh=mesh,
        in_specs=placed,
        out_specs=(
            P(None, None, None, "ta", "gx", "gy"),
            P(None, None, None, "ta", "gx", "gy"),
            P(None, "ta"),
            P("ta"),
        ),
        check_vma=False,
    )
```

```python
import math

import jax
import jax.numpy as jnp
from jax import lax
from jax.experimental import pallas as pl
from jax.experimental.pallas import tpu as pltpu
from jax.sharding import PartitionSpec as P


NZ = 48
ITERS = 4

OMEGA = 1.7
FLOOR = 0.5
PAIRS = ((0, 1), (1, 2), (0, 2))

LANES = 128
HALF = LANES // 2
BLOCK_ROWS = LANES // math.gcd(NZ, LANES)
TILES = BLOCK_ROWS * NZ // LANES
BLOCK = BLOCK_ROWS * NZ
WINDOW = 4
COORDS = 8
PARTS = 4 * COORDS
ROW_Y = COORDS
GAUGE_AT = 3 * COORDS
POLE = 1e15
NEAR_POLE = 1e-30


def to_plane(point):
    first, rest = point[0], point[1:]
    square = rest[0] * rest[0]
    for entry in rest[1:]:
        square = square + entry * entry
    upper = first >= 0.0
    top = jnp.where(upper, 1.0, 1.0 - first)
    bottom = jnp.where(upper, 1.0 + first, jnp.maximum(square, NEAR_POLE))
    scale = top / bottom
    plane = [scale * entry for entry in rest]
    at_pole = (first < 0.0) & (square < NEAR_POLE)
    plane[0] = jnp.where(at_pole, POLE, plane[0])
    return plane


def from_plane(plane):
    square = plane[0] * plane[0]
    for entry in plane[1:]:
        square = square + entry * entry
    scale = 2.0 / (1.0 + square)
    return scale, [scale - 1.0] + [scale * entry for entry in plane]


def row_and_basis(plane):
    scale, point = from_plane(plane)
    row = [(point[0], point[1]), (point[2], point[3]), (point[4], point[5])]
    u = [(scale, point[1]), row[1], row[2]]
    tilt = plane[0]
    inverse = 1.0 / (1.0 + tilt * tilt)
    basis = []
    for j in (1, 2):
        re, im = plane[2 * j - 1], plane[2 * j]
        zr = (re + im * tilt) * inverse
        zi = (re * tilt - im) * inverse
        vector = []
        for k in range(3):
            ur, ui = u[k]
            br = ui * zi - ur * zr
            bi = -(ur * zi + ui * zr)
            vector.append((1.0 + br, bi) if k == j else (br, bi))
        basis.append(vector)
    return row, basis


def encode(first, second):
    point = [part for entry in first for part in entry]
    plane = to_plane(point)
    _, basis = row_and_basis(plane)
    coeffs = []
    for vector in basis:
        re = im = None
        for (sr, si), (br, bi) in zip(second, vector):
            tr = sr * br + si * bi
            ti = si * br - sr * bi
            re = tr if re is None else re + tr
            im = ti if im is None else im + ti
        coeffs += [re, im]
    return plane + to_plane(coeffs)


def decode(coords):
    first, basis = row_and_basis(coords[:5])
    _, coeffs = from_plane(coords[5:])
    second = []
    for k in range(3):
        re = im = None
        for j in range(2):
            cr, ci = coeffs[2 * j], coeffs[2 * j + 1]
            br, bi = basis[j][k]
            tr = cr * br - ci * bi
            ti = cr * bi + ci * br
            re = tr if re is None else re + tr
            im = ti if im is None else im + ti
        second.append((re, im))
    third = []
    for i in range(3):
        (ar, ai), (cr, ci) = first[(i + 1) % 3], first[(i + 2) % 3]
        (br, bi), (dr, di) = second[(i + 1) % 3], second[(i + 2) % 3]
        re = (ar * dr - ai * di) - (cr * br - ci * bi)
        im = (cr * bi + ci * br) - (ar * di + ai * dr)
        third.append((re, im))
    rows = first + second + third
    return [entry[0] for entry in rows], [entry[1] for entry in rows]


def pack_kernel(
    own_tiles, links_hbm, gauge_hbm, own, below, above, links, gauge, natural, coded, arrived
):
    copies = [
        pltpu.make_async_copy(
            links_hbm.at[pl.ds(18 * axis, 18)], links.at[pl.ds(18 * axis, 18)], arrived.at[axis]
        )
        for axis in range(3)
    ]
    copies.append(pltpu.make_async_copy(gauge_hbm, gauge, arrived.at[3]))
    for copy in copies:
        copy.start()
    width = gauge.shape[-1]
    last = width - (own_tiles - 1) * LANES
    lane = lax.broadcasted_iota(jnp.int32, (2, width), 1)
    odd = (lane // NZ + lane % NZ) % 2 == 1
    rows = 2 * own_tiles
    for matrix in range(4):
        copies[matrix].wait()
        for number in range(12):
            entry = number if number < 6 else number + 3
            both = gauge[entry] if matrix == 3 else links[matrix * 18 + entry]
            swapped = jnp.concatenate([both[1:2], both[0:1]], axis=0)
            packed = jnp.where(odd, swapped, both)
            for t in range(own_tiles):
                tile = packed[:, t * LANES : (t + 1) * LANES]
                if t == own_tiles - 1:
                    tile = jnp.concatenate([tile, jnp.zeros((2, LANES - last), jnp.float32)], axis=1)
                natural[pl.ds((matrix * 12 + number) * rows + 2 * t, 2), :] = tile
        values = [natural[pl.ds((matrix * 12 + i) * rows, rows), :] for i in range(12)]
        entries = [(values[i], values[6 + i]) for i in range(6)]
        for i, value in enumerate(encode(entries[:3], entries[3:])):
            coded[pl.ds(8 + (matrix * COORDS + i) * rows, rows), :] = value
    low = lax.broadcasted_iota(jnp.int32, (rows, LANES), 1) < HALF
    first = own_tiles - 1 - TILES
    extra_below = extra_above = PARTS * TILES * 2
    for part in range(PARTS):
        base = 8 + part * rows
        here = pltpu.roll(coded[pl.ds(base, rows), :], HALF, 1)
        before = pltpu.roll(coded[pl.ds(base - 2, rows), :], HALF, 1)
        own[pl.ds(part * rows, rows), :] = jnp.where(low, before, here)
        at = part * TILES * 2
        edge = jnp.where(
            low[:2],
            coded[pl.ds(base + 2 * (own_tiles - 1), 2), :],
            coded[pl.ds(base + 2 * first, 2), :],
        )
        below[pl.ds(at, 2), :] = edge
        below[pl.ds(at + 2, 2 * TILES - 2), :] = coded[
            pl.ds(base + 2 * first + 2, 2 * TILES - 2), :
        ]
        above[pl.ds(at, 2 * TILES), :] = coded[pl.ds(base, 2 * TILES), :]
        if ROW_Y <= part < ROW_Y + COORDS or part >= GAUGE_AT:
            below[pl.ds(extra_below, 1), :] = coded[pl.ds(base + 2 * first + 1, 1), :]
            extra_below += 1
        if part >= GAUGE_AT:
            above[pl.ds(extra_above, 1), :] = coded[pl.ds(base + 2 * TILES + 1, 1), :]
            extra_above += 1


def pack(links, gauge):
    width = gauge.shape[-1]
    own_tiles = -(-width // LANES)
    rows = PARTS * TILES * 2
    shapes = [
        jax.ShapeDtypeStruct((PARTS * own_tiles * 2, LANES), jnp.float32),
        jax.ShapeDtypeStruct((rows + 2 * COORDS, LANES), jnp.float32),
        jax.ShapeDtypeStruct((rows + COORDS, LANES), jnp.float32),
    ]
    return pl.pallas_call(
        lambda *refs: pack_kernel(own_tiles, *refs),
        out_shape=shapes,
        in_specs=[pl.BlockSpec(memory_space=pltpu.HBM)] * 2,
        scratch_shapes=[
            pltpu.VMEM(links.shape, links.dtype),
            pltpu.VMEM(gauge.shape, gauge.dtype),
            pltpu.VMEM((48 * own_tiles * 2, LANES), jnp.float32),
            pltpu.VMEM((8 + PARTS * own_tiles * 2, LANES), jnp.float32),
            pltpu.SemaphoreType.DMA((4,)),
        ],
        compiler_params=pltpu.CompilerParams(vmem_limit_bytes=6 << 20),
        name="pack",
    )(*[pltpu.with_memory_space_constraint(value, pltpu.HBM) for value in (links, gauge)])


def row_roll(value, shift):
    return pltpu.roll(value, shift % value.shape[0], 0)


def lane_roll(value, shift):
    return pltpu.roll(value, shift % LANES, 1)


class Masks:
    def __init__(self, rows):
        self.lane = lax.broadcasted_iota(jnp.int32, (rows, LANES), 1)
        self.block = lax.broadcasted_iota(jnp.int32, (rows, LANES), 0) % WINDOW

    def z(self, tile):
        return (self.lane + tile * LANES) % NZ

    def odd(self, tile):
        return ((self.lane + tile * LANES) // NZ + self.z(tile)) % 2 == 1

    def owned(self, tile, start, width):
        place = self.block * BLOCK + tile * LANES + self.lane
        return (place >= start) & (place < start + width)


def y_ahead(tiles, masks):
    turned = [lane_roll(tile, -NZ) for tile in tiles]
    turned.append(row_roll(turned[0], -1))
    inside = masks.lane < LANES - NZ
    return [jnp.where(inside, turned[j], turned[j + 1]) for j in range(TILES)]


def y_behind(tiles, masks):
    turned = [lane_roll(tile, NZ) for tile in tiles]
    before = row_roll(turned[TILES - 1], 1)
    inside = masks.lane >= NZ
    return [jnp.where(inside, turned[j], turned[j - 1] if j else before) for j in range(TILES)]


def z_ahead(tiles, masks):
    step = [lane_roll(tile, -1) for tile in tiles]
    wrap = [lane_roll(tile, NZ - 1) for tile in tiles]
    out = []
    for j in range(TILES):
        near = step[j]
        if j < TILES - 1:
            near = jnp.where(masks.lane < LANES - 1, step[j], step[j + 1])
        far = wrap[j]
        if j:
            far = jnp.where(masks.lane >= NZ - 1, wrap[j], wrap[j - 1])
        out.append(jnp.where(masks.z(j) == NZ - 1, far, near))
    return out


def z_behind(tiles, masks):
    step = [lane_roll(tile, 1) for tile in tiles]
    wrap = [lane_roll(tile, 1 - NZ) for tile in tiles]
    out = []
    for j in range(TILES):
        near = step[j]
        if j:
            near = jnp.where(masks.lane >= 1, step[j], step[j - 1])
        far = wrap[j]
        if j < TILES - 1:
            far = jnp.where(masks.lane < LANES - NZ + 1, wrap[j], wrap[j + 1])
        out.append(jnp.where(masks.z(j) == 0, far, near))
    return out


def tile_of(j):
    return slice(j * LANES, (j + 1) * LANES)


def times_dagger(left, right):
    left_re, left_im = left
    right_re, right_im = right
    out_re = []
    out_im = []
    for a in range(3):
        for b in range(3):
            re = im = None
            for c in range(3):
                lr, li = left_re[3 * a + c], left_im[3 * a + c]
                rr, ri = right_re[3 * b + c], right_im[3 * b + c]
                re = lr * rr if re is None else re + lr * rr
                re = re + li * ri
                im = li * rr if im is None else im + li * rr
                im = im - lr * ri
            out_re.append(re)
            out_im.append(im)
    return out_re, out_im


def add_staple(sums, link, gauge):
    gauge_re, gauge_im = gauge
    both = [gauge_re[i] + gauge_im[i] for i in range(9)]
    right = (both, gauge_im, gauge_re)
    out = []
    for k in range(3):
        entries = []
        for a in range(3):
            for b in range(3):
                value = None if sums is None else sums[k][3 * a + b]
                for c in range(3):
                    term = link[k][3 * a + c] * right[k][3 * b + c]
                    value = term if value is None else value + term
                entries.append(value)
        out.append(entries)
    return out


def times(left, right):
    left_re, left_im = left
    right_re, right_im = right
    out_re = []
    out_im = []
    for a in range(3):
        for b in range(3):
            re = im = None
            for c in range(3):
                lr, li = left_re[3 * a + c], left_im[3 * a + c]
                rr, ri = right_re[3 * c + b], right_im[3 * c + b]
                re = lr * rr if re is None else re + lr * rr
                re = re - li * ri
                im = lr * ri if im is None else im + lr * ri
                im = im + li * rr
            out_re.append(re)
            out_im.append(im)
    return out_re, out_im


def relax_coeffs(moment, one, two):
    re, im = moment
    c0 = re[4 * one] + re[4 * two]
    c1 = -(im[3 * one + two] + im[3 * two + one])
    c2 = re[3 * two + one] - re[3 * one + two]
    c3 = im[4 * two] - im[4 * one]
    length = jnp.sqrt(c0 * c0 + c1 * c1 + c2 * c2 + c3 * c3)
    v0 = (1.0 - OMEGA) * length + OMEGA * c0
    v1 = OMEGA * c1
    v2 = OMEGA * c2
    v3 = OMEGA * c3
    scale = lax.rsqrt(jnp.maximum(v0 * v0 + v1 * v1 + v2 * v2 + v3 * v3, FLOOR * FLOOR))
    return v0 * scale, v1 * scale, v2 * scale, v3 * scale


def turn_rows(matrix, one, two, coeffs):
    a0, a1, a2, a3 = coeffs
    re = list(matrix[0])
    im = list(matrix[1])
    for col in range(3):
        f, s = 3 * one + col, 3 * two + col
        fr, fi, sr, si = re[f], im[f], re[s], im[s]
        re[f] = (a0 * fr - a3 * fi) + (a2 * sr - a1 * si)
        im[f] = (a0 * fi + a3 * fr) + (a2 * si + a1 * sr)
        re[s] = (a0 * sr + a3 * si) - (a2 * fr + a1 * fi)
        im[s] = (a0 * si - a3 * sr) + (a1 * fr - a2 * fi)
    return re, im


def antihermitian_squares(moment):
    re, im = moment
    total = None
    for a, b in PAIRS:
        dr = re[3 * a + b] - re[3 * b + a]
        di = im[3 * a + b] + im[3 * b + a]
        term = dr * dr + di * di
        total = term if total is None else total + term
    third = (im[0] + im[4] + im[8]) * (1.0 / 3.0)
    total = 0.5 * total
    for a in range(3):
        part = im[4 * a] - third
        total = total + part * part
    return total


def sweep_kernel(pairs, own_tiles, width, *refs):
    own = refs[0:pairs]
    below = refs[pairs : 2 * pairs]
    above = refs[2 * pairs : 3 * pairs]
    gauge_out, sums_out = refs[3 * pairs : 3 * pairs + 2]
    flat, extra, link, staple_link, field, moved, scores = refs[3 * pairs + 2 :]
    rows = pairs * WINDOW
    per_pair = WINDOW * TILES
    stride = pairs * per_pair
    start = width
    first_own = start // LANES
    masks = Masks(rows)

    for part in range(PARTS):
        for colour in range(2):
            for p in range(pairs):
                base = (colour * PARTS + part) * stride + p * per_pair
                flat[pl.ds(base + 1, TILES), :] = below[p][
                    pl.ds(part * TILES * 2 + colour, TILES, stride=2), :
                ]
                flat[pl.ds(base + first_own, own_tiles), :] = own[p][
                    pl.ds(part * own_tiles * 2 + colour, own_tiles, stride=2), :
                ]
                flat[pl.ds(base + per_pair - TILES, TILES), :] = above[p][
                    pl.ds(part * TILES * 2 + colour, TILES, stride=2), :
                ]
    for p in range(pairs):
        for i in range(2 * COORDS):
            extra[pl.ds(i * rows + WINDOW * p, 1), :] = below[p][pl.ds(PARTS * TILES * 2 + i, 1), :]
        for i in range(COORDS):
            ahead = WINDOW * ((p + 1) % pairs)
            extra[pl.ds((2 * COORDS + i) * rows + ahead, 1), :] = above[p][
                pl.ds(PARTS * TILES * 2 + i, 1), :
            ]

    first_block = masks.block == 0
    low_lanes = masks.lane < HALF
    low_second = (masks.block == 1) & low_lanes
    low_first = first_block & low_lanes

    def loaded(colour, part, j):
        base = (colour * PARTS + part) * stride
        value = flat[pl.ds(base + j, rows, stride=TILES), :]
        edge_y = ROW_Y <= part < ROW_Y + COORDS
        edge_g = part >= GAUGE_AT
        if j == 0:
            fill = jnp.zeros_like(value)
            if colour == 1 and edge_g:
                fill = extra[pl.ds((2 * COORDS + part - GAUGE_AT) * rows, rows), :]
            value = jnp.where(first_block, fill, value)
        if j == 1:
            value = jnp.where(low_second, row_roll(value, 1), value)
            if colour == 1 and (edge_y or edge_g):
                at = part - ROW_Y if edge_y else COORDS + part - GAUGE_AT
                value = jnp.where(low_first, extra[pl.ds(at * rows, rows), :], value)
        return value

    for colour in range(2):
        for matrix in range(4):
            target = link if matrix < 3 else field
            at = (colour * 3 + matrix) * 18 if matrix < 3 else colour * 18
            for j in range(TILES):
                coords = [loaded(colour, matrix * COORDS + i, j) for i in range(COORDS)]
                re, im = decode(coords)
                for i in range(9):
                    target[at + i, :, tile_of(j)] = re[i]
                    target[at + 9 + i, :, tile_of(j)] = im[i]

    def read(ref, at):
        return [ref[at, :, tile_of(j)] for j in range(TILES)]

    def write(ref, at, tiles):
        for j in range(TILES):
            ref[at, :, tile_of(j)] = tiles[j]

    def keep(colour, direction, entry, re, im):
        at = (colour * 6 + direction) * 27 + entry
        write(staple_link, at, re)
        write(staple_link, at + 9, [im[j] - re[j] for j in range(TILES)])
        write(staple_link, at + 18, [im[j] + re[j] for j in range(TILES)])

    for colour in range(2):
        for a in range(3):
            for c in range(3):
                here = 3 * a + c
                there = 3 * c + a
                same = []
                other = []
                for reim in range(2):
                    ours = read(link, colour * 3 * 18 + reim * 9 + here)
                    theirs = read(link, (1 - colour) * 3 * 18 + reim * 9 + there)
                    if reim:
                        theirs = [-t for t in theirs]
                    behind = [row_roll(t, WINDOW) for t in theirs]
                    lower = [masks.odd(j) if colour else ~masks.odd(j) for j in range(TILES)]
                    same.append([jnp.where(lower[j], ours[j], theirs[j]) for j in range(TILES)])
                    other.append([jnp.where(lower[j], behind[j], ours[j]) for j in range(TILES)])
                keep(colour, 0, here, *same)
                keep(colour, 1, here, *other)
                for axis, shift in ((1, y_behind), (2, z_behind)):
                    at = (colour * 3 + axis) * 18 + here
                    keep(colour, 2 * axis, here, read(link, at), read(link, at + 9))
                    at = ((1 - colour) * 3 + axis) * 18 + there
                    re = shift(read(link, at), masks)
                    im = [-t for t in shift(read(link, at + 9), masks)]
                    keep(colour, 2 * axis + 1, here, re, im)

    def move(colour):
        for i in range(18):
            tiles = read(field, colour * 18 + i)
            behind = [row_roll(t, WINDOW) for t in tiles]
            if 2 * WINDOW == rows:
                other = behind
            else:
                other = []
                for j in range(TILES):
                    lower = ~masks.odd(j) if colour else masks.odd(j)
                    other.append(jnp.where(lower, behind[j], row_roll(tiles[j], -WINDOW)))
            at = colour * 5 * 18 + i
            write(moved, at, other)
            write(moved, at + 18, y_ahead(tiles, masks))
            write(moved, at + 36, y_behind(tiles, masks))
            write(moved, at + 54, z_ahead(tiles, masks))
            write(moved, at + 72, z_behind(tiles, masks))

    def matrix_at(ref, at, group, j):
        block = [ref[at + i, group, tile_of(j)] for i in range(18)]
        return block[:9], block[9:]

    def moment_of(colour, group, j):
        them = 1 - colour
        sums = None
        for direction in range(6):
            if direction == 0:
                right = matrix_at(field, them * 18, group, j)
            else:
                right = matrix_at(moved, (them * 5 + direction - 1) * 18, group, j)
            at = (colour * 6 + direction) * 27
            entries = [staple_link[at + i, group, tile_of(j)] for i in range(27)]
            sums = add_staple(sums, (entries[:9], entries[9:18], entries[18:]), right)
        total = (
            [sums[0][i] + sums[1][i] for i in range(9)],
            [sums[2][i] - sums[0][i] for i in range(9)],
        )
        gauge = matrix_at(field, colour * 18, group, j)
        return gauge, times(gauge, total)

    def groups(body, init):
        count = rows // 8
        if count == 1:
            return body(0, pl.ds(0, 8), init)
        return lax.fori_loop(
            0, count, lambda g, carry: body(g, pl.ds(pl.multiple_of(g * 8, 8), 8), carry), init
        )

    group_masks = Masks(8)
    owned = [group_masks.owned(j, start, width) for j in range(TILES)]
    zero = jnp.zeros((8, LANES), jnp.float32)

    def half_sweep(colour, last=False):
        def body(g, group, carry):
            score, squares = carry
            for j in range(TILES):
                gauge, moment = moment_of(colour, group, j)
                for one, two in PAIRS:
                    coeffs = relax_coeffs(moment, one, two)
                    gauge = turn_rows(gauge, one, two, coeffs)
                    moment = turn_rows(moment, one, two, coeffs)
                for i in range(9):
                    field[colour * 18 + i, group, tile_of(j)] = gauge[0][i]
                    field[colour * 18 + 9 + i, group, tile_of(j)] = gauge[1][i]
                if colour == 1:
                    trace = moment[0][0] + moment[0][4] + moment[0][8]
                    score = score + jnp.where(owned[j], trace, 0.0)
                if last:
                    squares = squares + jnp.where(owned[j], antihermitian_squares(moment), 0.0)
            return score, squares

        return groups(body, (zero, zero))

    move(1)

    for k in range(ITERS):
        half_sweep(0)
        move(0)
        scores[k], scores[ITERS] = half_sweep(1, last=k == ITERS - 1)
        move(1)

    tile_line = lax.broadcasted_iota(jnp.int32, (own_tiles, LANES), 0)
    tile_lane = lax.broadcasted_iota(jnp.int32, (own_tiles, LANES), 1)
    place = tile_line * LANES + tile_lane
    odd = (place // NZ + place % NZ) % 2 == 1
    low = tile_lane < HALF
    for i in range(18):
        colours = []
        for colour in range(2):
            base = (colour * PARTS + i) * stride
            for j in range(TILES):
                flat[pl.ds(base + j, rows, stride=TILES), :] = field[colour * 18 + i, :, tile_of(j)]
            early = flat[pl.ds(base + first_own, own_tiles), :]
            late = flat[pl.ds(base + first_own + 1, own_tiles), :]
            colours.append(jnp.where(low, lane_roll(early, HALF), lane_roll(late, HALF)))
        planes = (
            jnp.where(odd, colours[1], colours[0]),
            jnp.where(odd, colours[0], colours[1]),
        )
        for x in range(2):
            for t in range(own_tiles):
                size = min(LANES, width - t * LANES)
                gauge_out[i, x : x + 1, t * LANES : t * LANES + size] = planes[x][
                    t : t + 1, :size
                ]

    def theta_body(g, group, squares):
        for j in range(TILES):
            _, moment = moment_of(0, group, j)
            squares = squares + jnp.where(owned[j], antihermitian_squares(moment), 0.0)
        return squares

    scores[ITERS] = groups(theta_body, scores[ITERS])

    line = lax.broadcasted_iota(jnp.int32, (8, LANES), 0)
    column = lax.broadcasted_iota(jnp.int32, (8, LANES), 1)
    sums = jnp.where(line == 1, jnp.sum(scores[ITERS]), 0.0)
    for k in range(ITERS):
        sums = jnp.where((line == 0) & (column == k), jnp.sum(scores[k]), sums)
    sums_out[...] = sums


def sweeps(own, below, above, width):
    pairs = len(own)
    own_tiles = -(-width // LANES)
    rows = pairs * WINDOW
    stride = pairs * WINDOW * TILES
    cells = lambda count: pltpu.VMEM((count, rows, BLOCK), jnp.float32)
    return pl.pallas_call(
        lambda *refs: sweep_kernel(pairs, own_tiles, width, *refs),
        out_shape=[
            jax.ShapeDtypeStruct((18, 2, width), jnp.float32),
            jax.ShapeDtypeStruct((8, LANES), jnp.float32),
        ],
        scratch_shapes=[
            pltpu.VMEM((2 * PARTS * stride, LANES), jnp.float32),
            pltpu.VMEM((3 * COORDS * rows, LANES), jnp.float32),
            cells(2 * 3 * 18),
            cells(2 * 6 * 27),
            cells(2 * 18),
            cells(2 * 5 * 18),
            pltpu.VMEM((8, 8, LANES), jnp.float32),
        ],
        compiler_params=pltpu.CompilerParams(vmem_limit_bytes=(pairs * 7 + 2) << 20),
        name="sweeps",
    )(*own, *below, *above)


def rotate_kernel(here, links, ahead, gauge, out):
    def matrix(ref):
        return [ref[i] for i in range(9)], [ref[9 + i] for i in range(9)]

    gauge[...] = here[...]
    re, im = times_dagger(times(matrix(here), matrix(links)), matrix(ahead))
    for i in range(9):
        out[i] = re[i]
        out[9 + i] = im[i]


def rotate(here, links, ahead):
    shape = jax.ShapeDtypeStruct(here.shape, here.dtype)
    return pl.pallas_call(
        rotate_kernel,
        out_shape=[shape, shape],
        compiler_params=pltpu.CompilerParams(vmem_limit_bytes=6 << 20),
        name="rotate",
    )(here, links, ahead)


def finish_kernel(volume, *refs):
    functional, theta = refs[-2:]
    total = refs[0][...]
    for part in refs[1:-2]:
        total = total + part[...]
    functional[...] = total[:1, :ITERS] * (1.0 / (9.0 * volume))
    theta[...] = total[1:2, :1] * (1.0 / (3.0 * volume))


def finish(parts, volume):
    return pl.pallas_call(
        lambda *refs: finish_kernel(volume, *refs),
        out_shape=[
            jax.ShapeDtypeStruct((1, ITERS), jnp.float32),
            jax.ShapeDtypeStruct((1, 1), jnp.float32),
        ],
        compiler_params=pltpu.CompilerParams(vmem_limit_bytes=1 << 20),
        name="finish",
    )(*parts)


def from_ahead(block, axis, distance):
    count = lax.axis_size(axis)
    return lax.ppermute(block, axis, [((i + distance) % count, i) for i in range(count)])


def fixed(space_links, time_links, start_gauge):
    x_sites, width = start_gauge.shape[-2:]
    pairs = lax.axis_size("gx")
    volume = x_sites * pairs * width * lax.axis_size("gy")
    assert x_sites == 2 and start_gauge.shape[3] == 1
    assert width % NZ == 0 and (width // NZ) % 2 == 0 and width % LANES == HALF
    assert 2 * width + BLOCK == WINDOW * BLOCK and pairs >= 2
    assert BLOCK_ROWS >= 2 * ITERS

    own, below, above = pack(
        space_links.reshape(54, x_sites, width), start_gauge.reshape(18, x_sites, width)
    )
    below = from_ahead(below, "gy", -1)
    above = from_ahead(above, "gy", 1)
    owns, belows, aboves = [own], [below], [above]
    for i in range(1, pairs):
        owns.append(from_ahead(own, "gx", i))
        belows.append(from_ahead(below, "gx", i))
        aboves.append(from_ahead(above, "gx", i))
    gauge, sums = sweeps(owns, belows, aboves, width)
    ahead = from_ahead(gauge, "ta", 1)
    count = lax.axis_size("gy")
    parts = [sums]
    for i in range(1, count):
        if count & (count - 1) == 0:
            parts.append(lax.ppermute(sums, "gy", [(k, k ^ i) for k in range(count)]))
        else:
            parts.append(from_ahead(sums, "gy", i))
    gauge, rotated = rotate(gauge, time_links.reshape(18, x_sites, width), ahead)
    functional, theta = finish(parts, volume)
    shape = start_gauge.shape
    return gauge.reshape(shape), rotated.reshape(shape), functional.reshape(ITERS, 1), theta.reshape(1)


def solution(mesh):
    placed = (
        P(None, None, None, None, "ta", "gx", "gy"),
        P(None, None, None, "ta", "gx", "gy"),
        P(None, None, None, "ta", "gx", "gy"),
    )
    return jax.shard_map(
        fixed,
        mesh=mesh,
        in_specs=placed,
        out_specs=(
            P(None, None, None, "ta", "gx", "gy"),
            P(None, None, None, "ta", "gx", "gy"),
            P(None, "ta"),
            P("ta"),
        ),
        check_vma=False,
    )
```
